32 devices in a mesh: grid: 8 (over z, y), band: 4 (over x, core).
Axes of the slice: x: 2, y: 2, z: 4, core: 2. Of those that a mesh axis runs over, the one named last changes fastest.
Arguments:
- orbitals: float32 [32, 16, 16, 512], P('grid', None, None, 'band'), may hold values from -80 to 80
- projectors: float32 [32, 16, 16, 512], P('grid', None, None, 'band'), may hold values from -0.09375 to 0.09375
- potential: float32 [32, 16, 16], P('grid'), may hold values from 0.3 to 3
Outputs:
- updated_orbitals: float32 [32, 16, 16, 512], P('grid', None, None, 'band')
- rayleigh_quotients: float32 [3, 512], P(None, 'band')
- residual_norms: float32 [3, 512], P(None, 'band')
The draws below stay inside these ranges and needn't reach their ends.
All inputs are finite; a program needn't handle non-finite values.
Results may differ from the reference program's by a relative error of at most 0.00012.
Values sent between devices are 32-bit elements; how exact they have to be, the bound alone decides.
A program may use at most 128 MiB of HBM per device.

```python
import math
import jax
import jax.numpy as jnp
from jax import lax

NX = 16
NY = 16
BANDS = 512
NXI = 512
ITERS = 3
NZ = 32


def draw_orbitals(key, part):
    jitter_key = jax.random.fold_in(key, 11)
    scale_key = jax.random.fold_in(key, 12)
    height = jnp.arange(NZ, dtype=jnp.float32) / max(NZ - 1, 1)
    scales = jnp.exp(jax.random.uniform(scale_key, (BANDS,), jnp.float32, 0.0, math.log(10.0)))
    profile = 0.6 + 1.2 * height
    jitter = jnp.clip(jax.random.normal(jitter_key, (NZ, NX, NY, BANDS), jnp.float32), -4.0, 4.0)
    values = jitter * profile[:, None, None, None] * scales
    return values.astype(jnp.float32)


def steps_of(key, extent, shards, smallest, top_value):
    def one(axis_at, shards_of):
        draws = jax.random.uniform(jax.random.fold_in(jax.random.fold_in(key, 6), axis_at), (shards_of,), jnp.float32, smallest / len(shards), top_value / len(shards))
        return jnp.repeat(jnp.exp(draws), extent[axis_at] // shards_of).reshape((-1,) + (1,) * (len(extent) - axis_at - 1))

    gain = one(*shards[0])
    for cut in shards[1:]:
        gain = gain * one(*cut)
    return gain


def scatter_about(key, shape, spread, bound, split=(), held_as=jnp.bfloat16):
    factor_of = steps_of(key, shape, split, -0.22, 0.18) if split else 1.0
    values = jax.random.normal(key, shape, jnp.float32) * spread * factor_of
    return jnp.minimum(jnp.maximum(values, -bound), bound).astype(held_as)


def setup_inputs(seed: int = 0) -> dict:
    splits = jax.random.split(jax.random.key(seed), 4)
    return {
        "orbitals": draw_orbitals(jax.random.fold_in(splits[3], 71), 0),
        "projectors": scatter_about(splits[1], (NZ, NX, NY, NXI), ((2.0 / (NZ * NX * NY)) ** 0.5), 0.09375, ((0, 8), (3, 4)), jnp.float32),
        "potential": jnp.clip(jnp.exp(math.log(3.0) - 2.3025851 * jax.random.uniform(splits[2], (NZ, NX, NY), jnp.float32) ** steps_of(splits[2], (NZ, NX, NY), ((0, 8),), -0.2, 0.2)), 0.3, 3.0),
    }


STENCIL = (-205.0 / 72.0, 8.0 / 5.0, -1.0 / 5.0, 8.0 / 315.0, -1.0 / 560.0)
STEP_LENGTH = 0.25
NORM_EPS = 1e-06
HIGHEST = lax.Precision.HIGHEST

def laplacian(grid_field):
    result = 3.0 * STENCIL[0] * grid_field
    for dimension in (0, 1, 2):
        for distance in range(1, 5):
            result = result + STENCIL[distance] * (jnp.roll(grid_field, distance, dimension) + jnp.roll(grid_field, -distance, dimension))
    return result

def matmul(left, right):
    return jnp.dot(left.astype(jnp.float32), right.astype(jnp.float32), precision=HIGHEST, preferred_element_type=jnp.float32)

def reference(orbitals, projectors, potential):
    grid_shape = orbitals.shape
    vectors = orbitals.reshape(-1, BANDS)
    projector_rows = projectors.reshape(-1, NXI)
    identity_matrix = jnp.eye(BANDS, dtype=jnp.float32)
    quotient_list = []
    norm_list = []
    for iteration in range(ITERS):
        margin = matmul(vectors.T, vectors)
        factor = jnp.linalg.cholesky(margin)
        inverse = jax.scipy.linalg.solve_triangular(factor, identity_matrix, lower=True)
        vectors = matmul(vectors, inverse.T)
        coupling = matmul(projector_rows.T, vectors)
        exchange_part = matmul(projector_rows, coupling)
        grid_field = vectors.reshape(grid_shape)
        applied = (-0.5 * laplacian(grid_field) + potential[..., None] * grid_field).reshape(-1, BANDS) - exchange_part
        rayleigh = lax.optimization_barrier(jnp.sum(vectors * applied, axis=0))
        residual = applied - rayleigh[None, :] * vectors
        squared = lax.optimization_barrier(jnp.sum(residual * residual, axis=0))
        vectors = vectors - STEP_LENGTH * residual / jnp.sqrt(squared + NORM_EPS)[None, :]
        quotient_list.append(rayleigh)
        norm_list.append(jnp.sqrt(squared))
    return (vectors.reshape(grid_shape), jnp.stack(quotient_list), jnp.stack(norm_list))
```

```python
import functools

import jax
import jax.numpy as jnp
from jax import lax
from jax.experimental import pallas as pl
from jax.experimental.pallas import tpu as pltpu
from jax.sharding import PartitionSpec as P

ITERS = 3


STENCIL = (-205.0 / 72.0, 8.0 / 5.0, -1.0 / 5.0, 8.0 / 315.0, -1.0 / 560.0)
STEP_LENGTH = 0.25
NORM_EPS = 1e-06
HIGHEST = lax.Precision.HIGHEST
MESH = pl.DeviceIdType.MESH
VMEM = pl.BlockSpec(memory_space=pltpu.VMEM)


def matmul(left, right, precision=HIGHEST):
    return jnp.dot(left, right, precision=precision, preferred_element_type=jnp.float32)


def laplacian(grid_field, low, high):
    padded = jnp.concatenate([low, grid_field, high], axis=0)
    planes_here = grid_field.shape[0]
    result = 3.0 * STENCIL[0] * grid_field
    for distance in range(1, 5):
        result = result + STENCIL[distance] * (
            padded[4 + distance : 4 + distance + planes_here]
            + padded[4 - distance : 4 - distance + planes_here]
        )
    for dimension in (1, 2):
        for distance in range(1, 5):
            result = result + STENCIL[distance] * (
                jnp.roll(grid_field, distance, dimension)
                + jnp.roll(grid_field, -distance, dimension)
            )
    return result


def dot_in_kernel(left, right, contract):
    return lax.dot_general(
        left, right, (contract, ((), ())), precision=HIGHEST, preferred_element_type=jnp.float32
    )


def block_inverse_factor(block, spread):
    size = block.shape[0]
    count = size // 8
    groups = [block[8 * g : 8 * g + 8, :] for g in range(count)]
    lane = lax.broadcasted_iota(jnp.int32, (8, size), 1)
    sublane = lax.broadcasted_iota(jnp.int32, (8, size), 0)

    def spread_column(value, j):
        return jnp.broadcast_to(value[:, j : j + 1], (8, size))

    finished = []
    for g in range(count):
        first = 8 * g
        slot = g % 2
        inside = (lane >= first) & (lane < first + 8)
        for t in range(8):
            spread[slot, 8 * t : 8 * t + 8, :] = spread_column(groups[g], first + t)
        start = jnp.where(inside, jnp.where(lane - first == sublane, 1.0, 0.0), groups[g])
        spread[slot, 64:72, :] = start

        def stored(at):
            return jnp.broadcast_to(spread[slot, at : at + 1, :], (8, size))

        entry = [[stored(8 * t + s) for t in range(s + 1)] for s in range(8)]
        rows = [stored(64 + s) for s in range(8)]
        following = g + 1 < count
        if following:
            ahead = [spread_column(groups[g + 1], first + t) for t in range(8)]
            value = jnp.where(inside, 0.0, groups[g + 1])
        inverse_pivot = []
        factor = [[None] * 8 for _ in range(8)]
        for t in range(8):
            inverse_pivot.append(1.0 / entry[t][t])
            for s in range(t + 1, 8):
                factor[s][t] = entry[s][t] * inverse_pivot[t]
                for u in range(t + 1, s + 1):
                    entry[s][u] = entry[s][u] - factor[s][t] * entry[u][t]
                rows[s] = rows[s] - factor[s][t] * rows[t]
                if following:
                    ahead[s] = ahead[s] - factor[s][t] * ahead[t]
            if following:
                value = value - (ahead[t] * inverse_pivot[t]) * rows[t]
        if following:
            groups[g + 1] = value
        result = jnp.zeros((8, size), jnp.float32)
        for s in range(8):
            result = jnp.where(sublane == s, rows[s] * (1.0 / jnp.sqrt(entry[s][s])), result)
        finished.append(jnp.where(lane < first + 8, result, 0.0))
        if g + 2 < count:
            solved = [None] * 8
            for s in reversed(range(8)):
                solved[s] = rows[s] * inverse_pivot[s]
                for t in range(s + 1, 8):
                    solved[s] = solved[s] - factor[t][s] * solved[t]
            for i in range(g + 2, count):
                value = jnp.where(inside, 0.0, groups[i])
                for t in range(8):
                    value = value - spread_column(groups[i], first + t) * solved[t]
                groups[i] = value
    return jnp.concatenate(finished, axis=0)


def inverse_factor_kernel(size, block, margin_ref, out_ref, work, panel, spread):
    work[...] = margin_ref[...]
    count = size // block

    @pl.loop(0, count)
    def _(k):
        here = pl.ds(pl.multiple_of(k * block, block), block)
        inverse = block_inverse_factor(work[here, here], spread)
        rows = dot_in_kernel(inverse, work[here, :], ((1,), (0,)))
        panel[...] = rows
        work[here, :] = rows
        work[here, here] = inverse

        @pl.loop(k + 1, count)
        def _(i):
            there = pl.ds(pl.multiple_of(i * block, block), block)
            work[there, here] = jnp.zeros((block, block), jnp.float32)
            work[there, :] = work[there, :] - dot_in_kernel(
                panel[:, there], work[here, :], ((0,), (0,))
            )

    for r in range(count):
        rows = pl.ds(r * block, block)
        out_ref[rows, :] = jnp.zeros((block, size), jnp.float32)
        out_ref[rows, : (r + 1) * block] = work[rows, : (r + 1) * block]


def inverse_factor(margin, block):
    size = margin.shape[0]
    return pl.pallas_call(
        functools.partial(inverse_factor_kernel, size, block),
        out_shape=jax.ShapeDtypeStruct((size, size), jnp.float32),
        in_specs=[VMEM], out_specs=VMEM,
        scratch_shapes=[pltpu.VMEM((size, size), jnp.float32), pltpu.VMEM((block, size), jnp.float32), pltpu.VMEM((2,72,block),jnp.float32)],
    )(margin)


def greet(axis, count, me):
    barrier = pltpu.get_barrier_semaphore()
    for k in range(1, count):
        pl.semaphore_signal(
            barrier, inc=1, device_id={axis: lax.rem(me + k, count)}, device_id_type=MESH
        )
    pl.semaphore_wait(barrier, count - 1)


def remote(axis, peer, source, target, send_sem, recv_sem):
    return pltpu.make_async_remote_copy(
        src_ref=source,
        dst_ref=target,
        send_sem=send_sem,
        recv_sem=recv_sem,
        device_id={axis: peer},
        device_id_type=MESH,
    )


def ring_places(count):
    me = lax.axis_index("band")
    half, side = lax.div(me, 2), lax.rem(me, 2)
    partner = half * 2 + 1 - side
    across = (1 - half) * 2 + side
    return me, partner, across, (1 - half) * 2 + 1 - side


def grid_sum_kernel(count, bands, edge, kind, *refs):
    refs = list(refs)
    x_ref = refs.pop(0)
    extra = refs.pop(0) if kind else None
    out_ref = refs.pop(0)
    extra_out = [refs.pop(0) for _ in range({"": 0, "gather": 1, "halo": 2}[kind])]
    parts, mine, total, s1, r1, s2, r2 = refs[:7]
    me = lax.axis_index("grid")
    chunk = x_ref.shape[0] // count
    barrier = pltpu.get_barrier_semaphore()
    for k in range(1, count):
        pl.semaphore_signal(
            barrier, inc=1, device_id={"grid": lax.rem(me + k, count)}, device_id_type=MESH
        )
    greeted = count - 1
    if kind == "gather":
        place, partner, across, opposite = ring_places(bands)
        for peer in (partner, across):
            pl.semaphore_signal(barrier, inc=1, device_id={"band": peer}, device_id_type=MESH)
        greeted += 2
    pl.semaphore_wait(barrier, greeted)
    if kind == "gather":
        held, send, recv = refs[7:]
        far = remote("band", across, extra, held.at[0], send.at[0], recv.at[0])
        near = remote("band", partner, extra, held.at[1], send.at[1], recv.at[1])
        far.start()
        near.start()
    copies = []
    for k in range(1, count):
        peer = lax.rem(me + k, count)
        copy = remote(
            "grid",
            peer,
            x_ref.at[pl.ds(pl.multiple_of(peer * chunk, chunk), chunk), :],
            parts.at[k - 1],
            s1.at[k - 1],
            r1.at[k - 1],
        )
        copy.start()
        copies.append(copy)
    if kind == "halo":
        held, send, recv = refs[7:]
        cells = extra.shape[0]
        after = remote(
            "grid",
            lax.rem(me + 1, count),
            extra.at[pl.ds(cells - edge, edge), :],
            held.at[0],
            send.at[0],
            recv.at[0],
        )
        before = remote(
            "grid",
            lax.rem(me + count - 1, count),
            extra.at[pl.ds(0, edge), :],
            held.at[1],
            send.at[1],
            recv.at[1],
        )
        after.start()
        before.start()
    own = pl.ds(pl.multiple_of(me * chunk, chunk), chunk)
    mine[...] = x_ref[own, :]
    for k in range(1, count):
        copies[k - 1].wait_recv()
        mine[...] += parts[k - 1]
    total[me] = mine[...]
    back = []
    for k in range(1, count):
        peer = lax.rem(me + k, count)
        copy = remote("grid", peer, mine, total.at[me], s2.at[k - 1], r2.at[k - 1])
        copy.start()
        back.append(copy)
    if kind == "gather":
        width = extra.shape[1]

        def put(source, value):
            extra_out[0][:, pl.ds(pl.multiple_of(source * width, width), width)] = value

        far.wait_recv()
        relay = remote("band", partner, held.at[0], held.at[2], send.at[2], recv.at[2])
        relay.start()
        put(place, extra[...])
        near.wait_recv()
        put(partner, held[1])
        put(across, held[0])
        relay.wait_recv()
        put(opposite, held[2])
        far.wait_send()
        near.wait_send()
        relay.wait_send()
    for k in range(1, count):
        copies[k - 1].wait_send()
        back[k - 1].wait()
    for c in range(count):
        out_ref[c * chunk : (c + 1) * chunk, :] = total[c]
    if kind == "halo":
        after.wait()
        before.wait()
        extra_out[0][...] = held[0]
        extra_out[1][...] = held[1]


def grid_sum(x, collective, kind="", extra=None, edge=0):
    count = lax.axis_size("grid")
    bands = lax.axis_size("band")
    rows, columns = x.shape
    chunk = rows // count
    sems = pltpu.SemaphoreType.DMA((count - 1,))
    out_shape = [jax.ShapeDtypeStruct(x.shape, jnp.float32)]
    more = []
    if kind == "gather":
        cells, width = extra.shape
        out_shape.append(jax.ShapeDtypeStruct((cells, width * bands), jnp.float32))
        more = [pltpu.VMEM((3, cells, width), jnp.float32)]
        more += [pltpu.SemaphoreType.DMA((3,))] * 2
    if kind == "halo":
        width = extra.shape[1]
        out_shape += [jax.ShapeDtypeStruct((edge, width), jnp.float32)] * 2
        more = [pltpu.VMEM((2, edge, width), jnp.float32)]
        more += [pltpu.SemaphoreType.DMA((2,))] * 2
    operands = [x] + ([extra] if kind else [])
    result = pl.pallas_call(
        functools.partial(grid_sum_kernel, count, bands, edge, kind),
        out_shape=out_shape,
        in_specs=[VMEM] * len(operands),
        out_specs=[VMEM] * len(out_shape),
        scratch_shapes=[
            pltpu.VMEM((count - 1, chunk, columns), jnp.float32),
            pltpu.VMEM((chunk, columns), jnp.float32),
            pltpu.VMEM((count, chunk, columns), jnp.float32),
            sems,
            sems,
            sems,
            sems,
        ]
        + more,
        compiler_params=pltpu.CompilerParams(collective_id=collective, has_side_effects=True),
        cost_estimate=pl.CostEstimate(flops=10**6, bytes_accessed=4 * 10**7, transcendentals=0),
    )(*operands)
    return result


def band_gather_kernel(count, x_ref, out_ref, held, send, recv):
    me = lax.axis_index("band")
    width = x_ref.shape[1]
    if count == 4:
        half, side = lax.div(me, 2), lax.rem(me, 2)
        partner = half * 2 + 1 - side
        across = (1 - half) * 2 + side
        barrier = pltpu.get_barrier_semaphore()
        for peer in (partner, across):
            pl.semaphore_signal(barrier, inc=1, device_id={"band": peer}, device_id_type=MESH)
        pl.semaphore_wait(barrier, 2)
        far = remote("band", across, x_ref, held.at[0], send.at[0], recv.at[0])
        far.start()
        near = remote("band", partner, x_ref, held.at[1], send.at[1], recv.at[1])
        near.start()
        out_ref[:, pl.ds(pl.multiple_of(me * width, width), width)] = x_ref[...]
        far.wait_recv()
        relay = remote("band", partner, held.at[0], held.at[2], send.at[2], recv.at[2])
        relay.start()
        near.wait_recv()
        out_ref[:, pl.ds(pl.multiple_of(partner * width, width), width)] = held[1]
        out_ref[:, pl.ds(pl.multiple_of(across * width, width), width)] = held[0]
        relay.wait_recv()
        opposite = (1 - half) * 2 + 1 - side
        out_ref[:, pl.ds(pl.multiple_of(opposite * width, width), width)] = held[2]
        far.wait_send()
        near.wait_send()
        relay.wait_send()
    else:
        greet("band", count, me)
        copies = []
        for k in range(1, count):
            peer = lax.rem(me + k, count)
            copy = remote("band", peer, x_ref, held.at[k - 1], send.at[k - 1], recv.at[k - 1])
            copy.start()
            copies.append(copy)
        out_ref[:, pl.ds(pl.multiple_of(me * width, width), width)] = x_ref[...]
        for k in range(1, count):
            copies[k - 1].wait()
            source = lax.rem(me + count - k, count)
            out_ref[:, pl.ds(pl.multiple_of(source * width, width), width)] = held[k - 1]


def band_gather(x, collective):
    count = lax.axis_size("band")
    rows, columns = x.shape
    return pl.pallas_call(
        functools.partial(band_gather_kernel, count),
        out_shape=jax.ShapeDtypeStruct((rows, columns * count), jnp.float32),
        in_specs=[VMEM],
        out_specs=VMEM,
        scratch_shapes=[
            pltpu.VMEM((count - 1, rows, columns), jnp.float32),
            pltpu.SemaphoreType.DMA((count - 1,)),
            pltpu.SemaphoreType.DMA((count - 1,)),
        ],
        compiler_params=pltpu.CompilerParams(collective_id=collective, has_side_effects=True),
        cost_estimate=pl.CostEstimate(flops=10**6, bytes_accessed=4 * 10**7, transcendentals=0),
    )(x)


def update_kernel(
    count, v_ref, w_ref, out_ref, quotient_ref, norm_ref, part1, part2, all1, all2, s1, r1, s2, r2
):
    me = lax.axis_index("grid")
    cells, bands = v_ref.shape
    greet("grid", count, me)

    def exchange(value, part, everyone, send, recv):
        part[...] = value
        everyone[me] = value
        copies = []
        for k in range(1, count):
            peer = lax.rem(me + k, count)
            copy = remote("grid", peer, part, everyone.at[me], send.at[k - 1], recv.at[k - 1])
            copy.start()
            copies.append(copy)
        for copy in copies:
            copy.wait()
        total = everyone[0]
        for c in range(1, count):
            total = total + everyone[c]
        return jnp.sum(total, axis=0, keepdims=True)

    products = v_ref[...] * w_ref[...]
    quotient = exchange(
        jnp.sum(products.reshape(cells // 8, 8, bands), axis=0), part1, all1, s1, r1
    )
    quotient_ref[...] = quotient
    residual = w_ref[...] - quotient * v_ref[...]
    squared = exchange(
        jnp.sum((residual * residual).reshape(cells // 8, 8, bands), axis=0), part2, all2, s2, r2
    )
    norm_ref[...] = jnp.sqrt(squared)
    factor = STEP_LENGTH / jnp.sqrt(squared + NORM_EPS)
    out_ref[...] = v_ref[...] - (w_ref[...] - quotient * v_ref[...]) * factor


def update(vectors, applied):
    count = lax.axis_size("grid")
    bands = vectors.shape[1]
    sems = pltpu.SemaphoreType.DMA((count - 1,))
    small = pltpu.VMEM((8, bands), jnp.float32)
    everyone = pltpu.VMEM((count, 8, bands), jnp.float32)
    line = jax.ShapeDtypeStruct((1, bands), jnp.float32)
    return pl.pallas_call(
        functools.partial(update_kernel, count),
        out_shape=(jax.ShapeDtypeStruct(vectors.shape, jnp.float32), line, line),
        in_specs=[VMEM, VMEM],
        out_specs=(VMEM, VMEM, VMEM),
        scratch_shapes=[small, small, everyone, everyone, sems, sems, sems, sems],
        compiler_params=pltpu.CompilerParams(collective_id=4, has_side_effects=True),
    )(vectors, applied)


def local(orbitals, projectors, potential):
    grid_shape = orbitals.shape
    local_bands = orbitals.shape[3]
    first_band = lax.axis_index("band") * local_bands
    vectors = orbitals.reshape(-1, local_bands)
    plane = vectors.shape[0] // grid_shape[0]
    projector_rows = projectors.reshape(-1, projectors.shape[3])
    joined = lax.axis_size("band") == 4
    if not joined:
        every_projector = band_gather(projector_rows, 3)
    quotient_list = []
    norm_list = []
    for iteration in range(ITERS):
        gathered = band_gather(vectors, 2)
        share = matmul(gathered.T, vectors)
        if iteration == 0 and joined:
            summed, every_projector = grid_sum(share, 5, "gather", projector_rows)
        else:
            (summed,) = grid_sum(share, 1)
        margin = band_gather(summed, 6)
        inverse = inverse_factor(margin, local_bands)
        rows = lax.dynamic_slice_in_dim(inverse, first_band, local_bands, 0)
        vectors = lax.dot_general(
            gathered,
            rows,
            (((1,), (1,)), ((), ())),
            precision=HIGHEST,
            preferred_element_type=jnp.float32,
        )
        coupling, low, high = grid_sum(
            matmul(every_projector.T, vectors, lax.Precision.HIGH), 7, "halo", vectors, 4 * plane
        )
        exchange_part = matmul(every_projector, coupling, lax.Precision.HIGH)
        grid_field = vectors.reshape(grid_shape)
        applied = (-0.5 * laplacian(
            grid_field, low.reshape(4, *grid_shape[1:]), high.reshape(4, *grid_shape[1:])
        ) + potential[..., None] * grid_field).reshape(
            -1, local_bands
        ) - exchange_part
        vectors, rayleigh, norm = update(vectors, applied)
        quotient_list.append(rayleigh)
        norm_list.append(norm)
    return (
        vectors.reshape(grid_shape),
        jnp.concatenate(quotient_list, axis=0),
        jnp.concatenate(norm_list, axis=0),
    )


def solution(mesh):
    return jax.shard_map(
        local,
        mesh=mesh,
        in_specs=(
            P("grid", None, None, "band"),
            P("grid", None, None, "band"),
            P("grid", None, None),
        ),
        out_specs=(P("grid", None, None, "band"), P(None, "band"), P(None, "band")),
        check_vma=False,
    )
```

```python
import functools

import jax
import jax.numpy as jnp
from jax import lax
from jax.experimental import pallas as pl
from jax.experimental.pallas import tpu as pltpu
from jax.sharding import PartitionSpec as P

ITERS = 3


STENCIL = (-205.0 / 72.0, 8.0 / 5.0, -1.0 / 5.0, 8.0 / 315.0, -1.0 / 560.0)
STEP_LENGTH = 0.25
NORM_EPS = 1e-06
HIGHEST = lax.Precision.HIGHEST
MESH = pl.DeviceIdType.MESH
VMEM = pl.BlockSpec(memory_space=pltpu.VMEM)
PIECES = 4
WIDE = 256
BF16 = jnp.bfloat16
F32 = jnp.float32


def exact_dot(left, right, contract):
    return lax.dot_general(
        left, right, (contract, ((), ())), precision=HIGHEST, preferred_element_type=F32
    )


def plain_dot(left, right, contract):
    return lax.dot_general(left, right, (contract, ((), ())), preferred_element_type=F32)


def split(value, parts):
    pieces = []
    for _ in range(parts - 1):
        head = value.astype(BF16)
        pieces.append(head)
        value = value - head.astype(F32)
    pieces.append(value.astype(BF16))
    return pieces


def split_dot(left, right, contract):
    total = None
    for order in reversed(range(max(len(left), len(right)))):
        for i in range(order + 1):
            if i < len(left) and order - i < len(right):
                term = plain_dot(left[i], right[order - i], contract)
                total = term if total is None else total + term
    return total


def block_inverse_factor(block, spread):
    size = block.shape[0]
    count = size // 8
    groups = [block[8 * g : 8 * g + 8, :] for g in range(count)]
    lane = lax.broadcasted_iota(jnp.int32, (8, size), 1)
    sublane = lax.broadcasted_iota(jnp.int32, (8, size), 0)

    def spread_column(value, j):
        return jnp.broadcast_to(value[:, j : j + 1], (8, size))

    finished = []
    for g in range(count):
        first = 8 * g
        slot = g % 2
        inside = (lane >= first) & (lane < first + 8)
        for t in range(8):
            spread[slot, 8 * t : 8 * t + 8, :] = spread_column(groups[g], first + t)
        start = jnp.where(inside, jnp.where(lane - first == sublane, 1.0, 0.0), groups[g])
        spread[slot, 64:72, :] = start

        def stored(at):
            return jnp.broadcast_to(spread[slot, at : at + 1, :], (8, size))

        entry = [[stored(8 * t + s) for t in range(s + 1)] for s in range(8)]
        rows = [stored(64 + s) for s in range(8)]
        following = g + 1 < count
        if following:
            ahead = [spread_column(groups[g + 1], first + t) for t in range(8)]
            value = jnp.where(inside, 0.0, groups[g + 1])
        inverse_pivot = []
        factor = [[None] * 8 for _ in range(8)]
        for t in range(8):
            inverse_pivot.append(1.0 / entry[t][t])
            for s in range(t + 1, 8):
                factor[s][t] = entry[s][t] * inverse_pivot[t]
                for u in range(t + 1, s + 1):
                    entry[s][u] = entry[s][u] - factor[s][t] * entry[u][t]
                rows[s] = rows[s] - factor[s][t] * rows[t]
                if following:
                    ahead[s] = ahead[s] - factor[s][t] * ahead[t]
            if following:
                value = value - (ahead[t] * inverse_pivot[t]) * rows[t]
        if following:
            groups[g + 1] = value
        result = jnp.zeros((8, size), F32)
        for s in range(8):
            result = jnp.where(sublane == s, rows[s] * (1.0 / jnp.sqrt(entry[s][s])), result)
        finished.append(jnp.where(lane < first + 8, result, 0.0))
        if g + 2 < count:
            solved = [None] * 8
            for s in reversed(range(8)):
                solved[s] = rows[s] * inverse_pivot[s]
                for t in range(s + 1, 8):
                    solved[s] = solved[s] - factor[t][s] * solved[t]
            for i in range(g + 2, count):
                value = jnp.where(inside, 0.0, groups[i])
                for t in range(8):
                    value = value - spread_column(groups[i], first + t) * solved[t]
                groups[i] = value
    return jnp.concatenate(finished, axis=0)


def remote(axis, peer, source, target, send_sem, recv_sem):
    return pltpu.make_async_remote_copy(
        src_ref=source,
        dst_ref=target,
        send_sem=send_sem,
        recv_sem=recv_sem,
        device_id={axis: peer},
        device_id_type=MESH,
    )


class BandGather:
    def __init__(self, source, target, place, sems):
        send, recv = sems
        me, partner, across = place
        self.copies = []
        rows = target.shape[2] // PIECES
        for q in range(PIECES):
            part = pl.ds(q * rows, rows)

            def block(owner, part=part):
                return target.at[owner, :, part, :]

            here = source.at[:, part, :]
            far = remote("band", across, here, block(me), send.at[0, q], recv.at[0, q])
            near = remote("band", partner, here, block(me), send.at[1, q], recv.at[1, q])
            relay = remote(
                "band", partner, block(across), block(across), send.at[2, q], recv.at[2, q]
            )
            self.copies.append((far, near, relay))

    def start(self):
        for far, _, _ in self.copies:
            far.start()
        for _, near, _ in self.copies:
            near.start()

    def pass_on(self):
        for far, _, relay in self.copies:
            far.wait_recv()
            relay.start()

    def finish(self):
        for far, near, relay in self.copies:
            near.wait_recv()
            relay.wait_recv()
        for far, near, relay in self.copies:
            far.wait_send()
            near.wait_send()
            relay.wait_send()


class GridSum:
    def __init__(self, part, arrived, mine, target, me, count, sems):
        s1, r1, s2, r2 = sems
        self.part, self.arrived, self.mine, self.target = part, arrived, mine, target
        chunk = mine.shape[0]
        self.own = pl.ds(pl.multiple_of(me * chunk, chunk), chunk)
        self.out, self.back = [], []
        for k in range(1, count):
            peer = lax.rem(me + k, count)
            there = pl.ds(pl.multiple_of(peer * chunk, chunk), chunk)
            self.out.append(
                remote("grid", peer, part.at[there, :], arrived.at[k - 1], s1.at[k - 1], r1.at[k - 1])
            )
            self.back.append(
                remote("grid", peer, mine, target.at[self.own, :], s2.at[k - 1], r2.at[k - 1])
            )

    def scatter(self):
        for copy in self.out:
            copy.start()

    def add(self):
        total = self.part[self.own, :]
        for k, copy in enumerate(self.out):
            copy.wait_recv()
            total = total + self.arrived[k]
        self.mine[...] = total
        for copy in self.back:
            copy.start()
        self.target[self.own, :] = total

    def finish(self):
        for copy in self.back:
            copy.wait_recv()
        for copy in self.out + self.back:
            copy.wait_send()


def iterations_kernel(count, bands, ny, *refs):
    (u0, x0, pot, out_ref, quot_ref, norm_ref) = refs[:6]
    (
        u, xr, kk, wb, uh, um, ul, xh, xm, kh, km, lh, lm, ll, work, panel, spread,
        spart, cpart, sin, cin, smine, cmine, csum, sall, hz, hs, hr, stat, stats, lam,
        sums_s, sums_c, gat_u, gat_x, gat_s, gat_k, halo_z, halo_y, stat_s, stat_r,
    ) = refs[6:]
    me = lax.axis_index("grid")
    band = lax.axis_index("band")
    half, side = lax.div(band, 2), lax.rem(band, 2)
    partner = half * 2 + 1 - side
    across = (1 - half) * 2 + side
    place = (band, partner, across)
    planes, plane, w = u0.shape
    n = planes * plane
    total = bands * w
    nx = plane // ny

    barrier = pltpu.get_barrier_semaphore()
    for k in range(1, count):
        pl.semaphore_signal(
            barrier, inc=1, device_id={"grid": lax.rem(me + k, count)}, device_id_type=MESH
        )
    for peer in (partner, across):
        pl.semaphore_signal(barrier, inc=1, device_id={"band": peer}, device_id_type=MESH)
    pl.semaphore_wait(barrier, count + 1)

    stat[...] = jnp.zeros_like(stat)
    gather_u = BandGather(u0, u, place, (gat_u.at[0], gat_u.at[1]))
    gather_x = BandGather(x0, xr, place, (gat_x.at[0], gat_x.at[1]))
    gather_u.start()
    gather_x.start()
    u[band] = u0[...]
    xr[band] = x0[...]
    gather_u.pass_on()
    gather_u.finish()

    odd = lax.rem(me, 2)
    z_peer = lax.rem(me + count + 4 * odd - 2, count)
    y_peer = me + 1 - 2 * odd
    part_rows = plane // PIECES

    def lanes(j):
        return slice(j * w, (j + 1) * w)

    def split_blocks(source, targets):
        for j in range(bands):
            @pl.loop(0, planes)
            def _(p):
                rows = pl.ds(pl.multiple_of(p * plane, plane), plane)
                for target, piece in zip(targets, split(source[j, p], len(targets))):
                    target[rows, lanes(j)] = piece

    def iteration(it):
        sum_s = GridSum(spart, sin, smine, sall.at[band], me, count, [sums_s.at[i] for i in range(4)])
        sum_c = GridSum(cpart, cin, cmine, csum, me, count, [sums_c.at[i] for i in range(4)])
        gather_s = BandGather(
            sall.at[band].reshape(1, total, w), sall.reshape(bands, 1, total, w), place,
            (gat_s.at[0], gat_s.at[1]),
        )
        gather_k = BandGather(kk.at[band], kk, place, (gat_k.at[0], gat_k.at[1]))
        across_z, across_y = [], []
        for q in range(PIECES):
            part = pl.ds(q * part_rows, part_rows)
            across_z.append(
                remote("grid", z_peer, u.at[band, :, part, :], hz.at[:, part, :],
                       halo_z.at[0, q], halo_z.at[1, q])
            )
            across_y.append(
                remote("grid", y_peer, hs.at[:, part, :], hr.at[:, part, :],
                       halo_y.at[0, q], halo_y.at[1, q])
            )

        across_z[0].start()
        split_blocks(u, (uh, um, ul))
        turned = split(jnp.transpose(u[band].reshape(n, w)), 3)
        for start in range(0, total, WIDE):
            wide = slice(start, start + WIDE)
            tile = split_dot(turned, [uh[:, wide], um[:, wide], ul[:, wide]], ((1,), (0,)))
            for c in range(WIDE // w):
                at = start + c * w
                spart[at : at + w, :] = tile[:, lanes(c)]
        sum_s.scatter()
        across_z[1].start()

        @pl.when(it == 0)
        def _():
            gather_x.pass_on()
            gather_x.finish()
            split_blocks(xr, (xh, xm))

        for start in range(0, total, WIDE):
            wide = slice(start, start + WIDE)
            tile = split_dot(turned[:2], [xh[:, wide], xm[:, wide]], ((1,), (0,)))
            for c in range(WIDE // w):
                at = start + c * w
                cpart[at : at + w, :] = tile[:, lanes(c)]

        def halo_part(q):
            across_z[q].wait_recv()
            for own_above in (0, 1):
                @pl.when(odd == own_above)
                def _():
                    @pl.loop(0, part_rows // 16)
                    def _(r):
                        rows = pl.ds(pl.multiple_of(q * part_rows + r * 16, 16), 16)
                        own = [u[band, j, rows, :] for j in range(planes)]
                        other = [hz[j, rows, :] for j in range(planes)]
                        below, above = (other, own) if own_above else (own, other)
                        for p in range(planes):
                            value = None
                            for d in range(1, 5):
                                terms = []
                                if p - d < 0:
                                    terms.append(below[planes + p - d])
                                if p + d >= planes:
                                    terms.append(above[p + d - planes])
                                for term in terms:
                                    term = STENCIL[d] * term
                                    value = term if value is None else value + term
                            hs[p, rows, :] = value
            across_y[q].start()

        sum_s.add()
        sum_c.scatter()
        across_z[2].start()
        across_z[3].start()
        halo_part(0)
        halo_part(1)

        @pl.loop(0, nx)
        def _(x):
            def rows_at(at):
                return pl.ds(pl.multiple_of(lax.rem(at + nx, nx) * ny, ny), ny)

            rows = rows_at(x)
            field = [u[band, p, rows, :] for p in range(planes)]
            for p in range(planes):
                value = 3.0 * STENCIL[0] * field[p]
                for d in range(1, 5):
                    near = u[band, p, rows_at(x + d), :] + u[band, p, rows_at(x - d), :]
                    near = near + pltpu.roll(field[p], d, 0) + pltpu.roll(field[p], ny - d, 0)
                    if p - d >= 0:
                        near = near + field[p - d]
                    if p + d < planes:
                        near = near + field[p + d]
                    value = value + STENCIL[d] * near
                kk[band, p, rows, :] = -0.5 * value + pot[p, rows, :] * field[p]

        sum_s.finish()
        gather_s.start()
        halo_part(2)
        halo_part(3)
        sum_c.add()
        gather_s.pass_on()
        gather_s.finish()
        for b in range(bands):
            for c in range(bands):
                work[b * w : (b + 1) * w, lanes(c)] = sall[b, c * w : (c + 1) * w, :]

        def exchange_and_send():
            sum_c.finish()
            coupling = jnp.concatenate(
                [jnp.transpose(csum[c * w : (c + 1) * w, :]) for c in range(bands)], axis=0
            )
            right = split(coupling, 2)
            for copy in across_y:
                copy.wait_recv()

            @pl.loop(0, planes)
            def _(p):
                rows = pl.ds(pl.multiple_of(p * plane, plane), plane)
                exchange = split_dot([xh[rows, :], xm[rows, :]], right, ((1,), (0,)))
                kk[band, p] = kk[band, p] - 0.5 * hr[p] - exchange
            gather_k.start()

        @pl.loop(0, bands)
        def _(k):
            here = pl.ds(pl.multiple_of(k * w, w), w)
            inverse = block_inverse_factor(work[here, here], spread)
            rows = exact_dot(inverse, work[here, :], ((1,), (0,)))
            panel[...] = rows
            work[here, :] = rows
            work[here, here] = inverse

            @pl.loop(k + 1, bands)
            def _(i):
                there = pl.ds(pl.multiple_of(i * w, w), w)
                work[there, here] = jnp.zeros((w, w), F32)
                work[there, :] = work[there, :] - exact_dot(
                    panel[:, there], work[here, :], ((0,), (0,))
                )

            @pl.when(k == 1)
            def _():
                exchange_and_send()

        gather_k.pass_on()
        for r in range(bands):
            rows = slice(r * w, (r + 1) * w)
            for target, piece in zip((lh, lm, ll), split(work[rows, :], 3)):
                target[rows, : (r + 1) * w] = piece[:, : (r + 1) * w]
                if (r + 1) * w < total:
                    target[rows, (r + 1) * w :] = jnp.zeros((w, total - (r + 1) * w), BF16)
        gather_k.finish()
        split_blocks(kk, (kh, km))
        for copy in across_z + across_y:
            copy.wait_send()

        @pl.loop(0, planes)
        def _(p):
            rows = pl.ds(pl.multiple_of(p * plane, plane), plane)
            for start in range(0, total, WIDE):
                deep = slice(0, start + WIDE)
                wide = slice(start, start + WIDE)
                right = [lh[wide, deep], lm[wide, deep], ll[wide, deep]]
                v = split_dot([uh[rows, deep], um[rows, deep], ul[rows, deep]], right, ((1,), (1,)))
                t = split_dot([kh[rows, deep], km[rows, deep]], right[:2], ((1,), (1,)))
                for c in range(WIDE // w):
                    u[start // w + c, p] = v[:, lanes(c)]
                    wb[start // w + c, p] = t[:, lanes(c)]

        def column_sum(value):
            return jnp.sum(value, axis=0, keepdims=True)

        def eight(value):
            return jnp.sum(value.reshape(plane // 8, 8, w), axis=0)

        for j in range(bands):
            zero = jnp.zeros((8, w), F32)

            def first(p, carry, j=j):
                v, t = u[j, p], wb[j, p]
                return carry[0] + eight(v * t), carry[1] + eight(v * v)

            vw, vv = lax.fori_loop(0, planes, first, (zero, zero))
            vw, vv = column_sum(vw), column_sum(vv)
            slope = jnp.where(vv > 1e-12, vw / jnp.maximum(vv, 1e-12), 0.0)

            def second(p, carry, j=j, slope=slope):
                r = wb[j, p] - slope * u[j, p]
                return carry + eight(r * r)

            rest = column_sum(lax.fori_loop(0, planes, second, zero))
            stat[j : j + 1, :] = vw
            stat[bands + j : bands + j + 1, :] = vv
            stat[2 * bands + j : 2 * bands + j + 1, :] = rest

        copies = []
        for k in range(1, count):
            peer = lax.rem(me + k, count)
            copy = remote("grid", peer, stat, stats.at[me], stat_s.at[k - 1], stat_r.at[k - 1])
            copy.start()
            copies.append(copy)
        stats[me] = stat[...]
        for copy in copies:
            copy.wait()
        quotient = stats[0, :bands, :]
        for c in range(1, count):
            quotient = quotient + stats[c, :bands, :]
        squared = jnp.zeros((bands, w), F32)
        for c in range(count):
            vw, vv = stats[c, :bands, :], stats[c, bands : 2 * bands, :]
            slope = jnp.where(vv > 1e-12, vw / jnp.maximum(vv, 1e-12), 0.0)
            shift = slope - quotient
            squared = squared + stats[c, 2 * bands : 3 * bands, :]
            squared = squared + shift * (2.0 * (vw - slope * vv) + shift * vv)
        squared = jnp.maximum(squared, 0.0)
        lam[0, :bands, :] = quotient
        lam[1, :bands, :] = jnp.sqrt(squared)
        lam[2, :bands, :] = STEP_LENGTH / jnp.sqrt(squared + NORM_EPS)
        quot_ref[pl.ds(it, 1), :] = lam[0, pl.ds(band, 1), :]
        norm_ref[pl.ds(it, 1), :] = lam[1, pl.ds(band, 1), :]
        for j in range(bands):
            rate, length = lam[0, j : j + 1, :], lam[2, j : j + 1, :]

            @pl.loop(0, planes)
            def _(p, j=j, rate=rate, length=length):
                v = u[j, p]
                u[j, p] = v - (wb[j, p] - rate * v) * length

    @pl.loop(0, ITERS)
    def _(it):
        iteration(it)

    out_ref[...] = u[band]


def local(orbitals, projectors, potential):
    grid_shape = orbitals.shape
    planes, nx, ny, w = grid_shape
    plane = nx * ny
    n = planes * plane
    count = lax.axis_size("grid")
    bands = lax.axis_size("band")
    total = bands * w
    chunk = total // count
    field = (planes, plane, w)
    block = pltpu.VMEM((bands,) + field, F32)
    half = pltpu.VMEM((n, total), BF16)
    square = pltpu.VMEM((total, total), BF16)
    column = pltpu.VMEM((total, w), F32)
    arrived = pltpu.VMEM((count - 1, chunk, w), F32)
    mine = pltpu.VMEM((chunk, w), F32)
    slab = pltpu.VMEM(field, F32)
    dma = pltpu.SemaphoreType.DMA
    spread_potential = jnp.broadcast_to(potential.reshape(planes, plane, 1), field)
    line = jax.ShapeDtypeStruct((ITERS, w), F32)
    updated, quotients, norms = pl.pallas_call(
        functools.partial(iterations_kernel, count, bands, ny),
        out_shape=(jax.ShapeDtypeStruct(field, F32), line, line),
        in_specs=[VMEM] * 3,
        out_specs=(VMEM, VMEM, VMEM),
        scratch_shapes=[block] * 4
        + [half] * 7
        + [square] * 3
        + [
            pltpu.VMEM((total, total), F32),
            pltpu.VMEM((w, total), F32),
            pltpu.VMEM((2, 72, w), F32),
        ]
        + [column, column, arrived, arrived, mine, mine, column]
        + [pltpu.VMEM((bands, total, w), F32), slab, slab, slab]
        + [
            pltpu.VMEM((16, w), F32),
            pltpu.VMEM((count, 16, w), F32),
            pltpu.VMEM((3, 8, w), F32),
        ]
        + [dma((4, count - 1))] * 2
        + [dma((2, 3, PIECES))] * 4
        + [dma((2, PIECES))] * 2
        + [dma((count - 1,))] * 2,
        compiler_params=pltpu.CompilerParams(
            collective_id=0, has_side_effects=True, vmem_limit_bytes=60 * 2**20
        ),
    )(orbitals.reshape(field), projectors.reshape(field), spread_potential)
    return updated.reshape(grid_shape), quotients, norms


def solution(mesh):
    return jax.shard_map(
        local,
        mesh=mesh,
        in_specs=(
            P("grid", None, None, "band"),
            P("grid", None, None, "band"),
            P("grid", None, None),
        ),
        out_specs=(P("grid", None, None, "band"), P(None, "band"), P(None, "band")),
        check_vma=False,
    )
```

```python
import functools

import jax
import jax.numpy as jnp
from jax import lax
from jax.experimental import pallas as pl
from jax.experimental.pallas import tpu as pltpu
from jax.sharding import PartitionSpec as P

ITERS = 3


STENCIL = (-205.0 / 72.0, 8.0 / 5.0, -1.0 / 5.0, 8.0 / 315.0, -1.0 / 560.0)
STEP_LENGTH = 0.25
NORM_EPS = 1e-06
HIGHEST = lax.Precision.HIGHEST
MESH = pl.DeviceIdType.MESH
VMEM = pl.BlockSpec(memory_space=pltpu.VMEM)
PIECES = 4
WIDE = 256
BF16 = jnp.bfloat16
F32 = jnp.float32


def exact_dot(left, right, contract):
    return lax.dot_general(
        left, right, (contract, ((), ())), precision=HIGHEST, preferred_element_type=F32
    )


def plain_dot(left, right, contract):
    return lax.dot_general(left, right, (contract, ((), ())), preferred_element_type=F32)


def split(value, parts):
    pieces = []
    for _ in range(parts - 1):
        head = value.astype(BF16)
        pieces.append(head)
        value = value - head.astype(F32)
    pieces.append(value.astype(BF16))
    return pieces


def split_dot(left, right, contract):
    total = None
    for order in reversed(range(max(len(left), len(right)))):
        for i in range(order + 1):
            if i < len(left) and order - i < len(right):
                term = plain_dot(left[i], right[order - i], contract)
                total = term if total is None else total + term
    return total


def block_inverse_factor(block, spread):
    size = block.shape[0]
    count = size // 8
    groups = [block[8 * g : 8 * g + 8, :] for g in range(count)]
    lane = lax.broadcasted_iota(jnp.int32, (8, size), 1)
    sublane = lax.broadcasted_iota(jnp.int32, (8, size), 0)

    def spread_column(value, j):
        return jnp.broadcast_to(value[:, j : j + 1], (8, size))

    finished = []
    for g in range(count):
        first = 8 * g
        slot = g % 2
        inside = (lane >= first) & (lane < first + 8)
        for t in range(8):
            spread[slot, 8 * t : 8 * t + 8, :] = spread_column(groups[g], first + t)
        start = jnp.where(inside, jnp.where(lane - first == sublane, 1.0, 0.0), groups[g])
        spread[slot, 64:72, :] = start

        def stored(at):
            return jnp.broadcast_to(spread[slot, at : at + 1, :], (8, size))

        entry = [[stored(8 * t + s) for t in range(s + 1)] for s in range(8)]
        rows = [stored(64 + s) for s in range(8)]
        following = g + 1 < count
        if following:
            ahead = [spread_column(groups[g + 1], first + t) for t in range(8)]
            value = jnp.where(inside, 0.0, groups[g + 1])
        inverse_pivot = []
        factor = [[None] * 8 for _ in range(8)]
        for t in range(8):
            inverse_pivot.append(1.0 / entry[t][t])
            for s in range(t + 1, 8):
                factor[s][t] = entry[s][t] * inverse_pivot[t]
                for u in range(t + 1, s + 1):
                    entry[s][u] = entry[s][u] - factor[s][t] * entry[u][t]
                rows[s] = rows[s] - factor[s][t] * rows[t]
                if following:
                    ahead[s] = ahead[s] - factor[s][t] * ahead[t]
            if following:
                value = value - (ahead[t] * inverse_pivot[t]) * rows[t]
        if following:
            groups[g + 1] = value
        result = jnp.zeros((8, size), F32)
        for s in range(8):
            result = jnp.where(sublane == s, rows[s] * (1.0 / jnp.sqrt(entry[s][s])), result)
        finished.append(jnp.where(lane < first + 8, result, 0.0))
        if g + 2 < count:
            solved = [None] * 8
            for s in reversed(range(8)):
                solved[s] = rows[s] * inverse_pivot[s]
                for t in range(s + 1, 8):
                    solved[s] = solved[s] - factor[t][s] * solved[t]
            for i in range(g + 2, count):
                value = jnp.where(inside, 0.0, groups[i])
                for t in range(8):
                    value = value - spread_column(groups[i], first + t) * solved[t]
                groups[i] = value
    return jnp.concatenate(finished, axis=0)


def remote(axis, peer, source, target, send_sem, recv_sem):
    return pltpu.make_async_remote_copy(
        src_ref=source,
        dst_ref=target,
        send_sem=send_sem,
        recv_sem=recv_sem,
        device_id={axis: peer},
        device_id_type=MESH,
    )


class BandGather:
    def __init__(self, source, target, place, sems):
        send, recv = sems
        me, partner, across = place
        self.copies = []
        rows = target.shape[2] // PIECES
        for q in range(PIECES):
            part = pl.ds(q * rows, rows)

            def block(owner, part=part):
                return target.at[owner, :, part, :]

            here = source.at[:, part, :]
            far = remote("band", across, here, block(me), send.at[0, q], recv.at[0, q])
            near = remote("band", partner, here, block(me), send.at[1, q], recv.at[1, q])
            relay = remote(
                "band", partner, block(across), block(across), send.at[2, q], recv.at[2, q]
            )
            self.copies.append((far, near, relay))

    def start(self):
        for far, _, _ in self.copies:
            far.start()
        for _, near, _ in self.copies:
            near.start()

    def pass_on(self, first=0, last=PIECES):
        for far, _, relay in self.copies[first:last]:
            far.wait_recv()
            relay.start()

    def finish(self):
        for far, near, relay in self.copies:
            near.wait_recv()
            relay.wait_recv()
        for far, near, relay in self.copies:
            far.wait_send()
            near.wait_send()
            relay.wait_send()


def far_first(me, count):
    low = 2 * me < count
    peers = []
    for k in range(count - 1):
        down = count - 1 - k
        down = jnp.where(down > me, down, down - 1)
        up = jnp.where(k < me, k, k + 1)
        peers.append(jnp.where(low, down, up))
    return peers


class GridSum:
    def __init__(self, part, paired, arrived, middle, target, me, count, sems):
        pair_s, pair_r, far_s, far_r, back_s, back_r, pass_s, pass_r = sems
        self.part, self.paired, self.arrived, self.held, self.target = (
            part, paired, arrived, middle, target,
        )
        chunk = middle.shape[1]
        half = count // 2
        place, side = lax.div(me, 2), lax.rem(me, 2)
        pair = me + 1 - 2 * side
        self.order = far_first(place, half) + [place]
        self.last = half - 1

        def rows(parity, owner):
            return pl.ds(pl.multiple_of((parity * half + owner) * chunk, chunk), chunk)

        self.mine = [rows(side, owner) for owner in self.order]
        self.pairs, self.far, self.far_in, self.back, self.back_in, self.passed = [], [], [], [], [], []
        own = middle.at[self.last]
        for j, owner in enumerate(self.order):
            theirs = part.at[rows(1 - side, owner), :]
            self.pairs.append(
                remote("grid", pair, theirs, paired.at[j], pair_s.at[j], pair_r.at[j])
            )
            done = target.at[self.mine[j], :]
            source = own if j == self.last else done
            self.passed.append(remote("grid", pair, source, done, pass_s.at[j], pass_r.at[j]))
            if j == self.last:
                continue
            peer = 2 * owner + side
            here = middle.at[j]
            self.far.append(
                remote("grid", peer, here, arrived.at[place], far_s.at[j], far_r.at[place])
            )
            self.far_in.append(
                remote("grid", peer, here, arrived.at[owner], far_s.at[j], far_r.at[owner])
            )
            home = target.at[rows(side, place), :]
            self.back.append(remote("grid", peer, own, home, back_s.at[j], back_r.at[place]))
            self.back_in.append(remote("grid", peer, own, done, back_s.at[j], back_r.at[owner]))

    def scatter(self):
        for copy in self.pairs:
            copy.start()

    def middle(self):
        for j, copy in enumerate(self.pairs):
            copy.wait_recv()
            self.held[j] = self.part[self.mine[j], :] + self.paired[j]
            if j < self.last:
                self.far[j].start()

    def add(self):
        total = self.held[self.last]
        for j in reversed(range(self.last)):
            self.far_in[j].wait_recv()
            total = total + self.arrived[self.order[j]]
        self.held[self.last] = total
        for copy in self.back:
            copy.start()
        self.passed[self.last].start()
        self.target[self.mine[self.last], :] = total

    def relay(self):
        for j in reversed(range(self.last)):
            self.back_in[j].wait_recv()
            self.passed[j].start()

    def finish(self):
        for copy in reversed(self.passed):
            copy.wait_recv()
        for copy in self.pairs + self.far + self.back + self.passed:
            copy.wait_send()


def iterations_kernel(count, bands, ny, *refs):
    (u0, x0, pot, out_ref, quot_ref, norm_ref) = refs[:6]
    (
        u, xr, kk, wb, uh, um, ul, xh, xm, kh, km, lh, lm, ll, work, panel, spread,
        spart, cpart, spair, cpair, sin, cin, smid, cmid, csum, sall, hz, hs, hr, stat, stats, lam,
        sums_s, sums_c, gat_u, gat_x, gat_s, gat_k, halo_z, halo_y, stat_s, stat_r,
    ) = refs[6:]
    me = lax.axis_index("grid")
    band = lax.axis_index("band")
    half, side = lax.div(band, 2), lax.rem(band, 2)
    partner = half * 2 + 1 - side
    across = (1 - half) * 2 + side
    place = (band, partner, across)
    planes, plane, w = u0.shape
    n = planes * plane
    total = bands * w
    nx = plane // ny

    barrier = pltpu.get_barrier_semaphore()
    for k in range(1, count):
        pl.semaphore_signal(
            barrier, inc=1, device_id={"grid": lax.rem(me + k, count)}, device_id_type=MESH
        )
    for peer in (partner, across):
        pl.semaphore_signal(barrier, inc=1, device_id={"band": peer}, device_id_type=MESH)
    pl.semaphore_wait(barrier, count + 1)

    stat[...] = jnp.zeros_like(stat)
    gather_u = BandGather(u0, u, place, (gat_u.at[0], gat_u.at[1]))
    gather_x = BandGather(x0, xr, place, (gat_x.at[0], gat_x.at[1]))
    gather_u.start()
    gather_x.start()
    u[band] = u0[...]
    xr[band] = x0[...]
    gather_u.pass_on()
    gather_u.finish()

    peers = far_first(me, count)
    odd = lax.rem(me, 2)
    z_peer = lax.rem(me + count + 4 * odd - 2, count)
    y_peer = me + 1 - 2 * odd
    part_rows = plane // PIECES

    def lanes(j):
        return slice(j * w, (j + 1) * w)

    def split_blocks(source, targets):
        for j in range(bands):
            @pl.loop(0, planes)
            def _(p):
                rows = pl.ds(pl.multiple_of(p * plane, plane), plane)
                for target, piece in zip(targets, split(source[j, p], len(targets))):
                    target[rows, lanes(j)] = piece

    def iteration(it):
        sum_s = GridSum(spart, spair, sin, smid, sall.at[band], me, count, [sums_s.at[i] for i in range(8)])
        sum_c = GridSum(cpart, cpair, cin, cmid, csum, me, count, [sums_c.at[i] for i in range(8)])
        gather_s = BandGather(
            sall.at[band].reshape(1, total, w), sall.reshape(bands, 1, total, w), place,
            (gat_s.at[0], gat_s.at[1]),
        )
        gather_k = BandGather(kk.at[band], kk, place, (gat_k.at[0], gat_k.at[1]))
        across_z, across_y = [], []
        for q in range(PIECES):
            part = pl.ds(q * part_rows, part_rows)
            across_z.append(
                remote("grid", z_peer, u.at[band, :, part, :], hz.at[:, part, :],
                       halo_z.at[0, q], halo_z.at[1, q])
            )
            across_y.append(
                remote("grid", y_peer, hs.at[:, part, :], hr.at[:, part, :],
                       halo_y.at[0, q], halo_y.at[1, q])
            )

        across_z[0].start()
        split_blocks(u, (uh, um, ul))
        turned = split(jnp.transpose(u[band].reshape(n, w)), 3)
        for start in range(0, total, WIDE):
            wide = slice(start, start + WIDE)
            tile = split_dot(turned, [uh[:, wide], um[:, wide], ul[:, wide]], ((1,), (0,)))
            for c in range(WIDE // w):
                at = start + c * w
                spart[at : at + w, :] = tile[:, lanes(c)]
        sum_s.scatter()

        @pl.when(it == 0)
        def _():
            gather_x.pass_on()
            gather_x.finish()
            split_blocks(xr, (xh, xm))

        for start in range(0, total, WIDE):
            wide = slice(start, start + WIDE)
            tile = split_dot(turned[:2], [xh[:, wide], xm[:, wide]], ((1,), (0,)))
            for c in range(WIDE // w):
                at = start + c * w
                cpart[at : at + w, :] = tile[:, lanes(c)]

        @pl.loop(0, nx)
        def _(x):
            def rows_at(at):
                return pl.ds(pl.multiple_of(lax.rem(at + nx, nx) * ny, ny), ny)

            rows = rows_at(x)
            field = [u[band, p, rows, :] for p in range(planes)]
            for p in range(planes):
                value = 3.0 * STENCIL[0] * field[p]
                for d in range(1, 5):
                    near = u[band, p, rows_at(x + d), :] + u[band, p, rows_at(x - d), :]
                    near = near + pltpu.roll(field[p], d, 0) + pltpu.roll(field[p], ny - d, 0)
                    if p - d >= 0:
                        near = near + field[p - d]
                    if p + d < planes:
                        near = near + field[p + d]
                    value = value + STENCIL[d] * near
                kk[band, p, rows, :] = -0.5 * value + pot[p, rows, :] * field[p]

        def halo_part(q):
            across_z[q].wait_recv()
            for own_above in (0, 1):
                @pl.when(odd == own_above)
                def _():
                    @pl.loop(0, part_rows // 16)
                    def _(r):
                        rows = pl.ds(pl.multiple_of(q * part_rows + r * 16, 16), 16)
                        own = [u[band, j, rows, :] for j in range(planes)]
                        other = [hz[j, rows, :] for j in range(planes)]
                        below, above = (other, own) if own_above else (own, other)
                        for p in range(planes):
                            value = None
                            for d in range(1, 5):
                                terms = []
                                if p - d < 0:
                                    terms.append(below[planes + p - d])
                                if p + d >= planes:
                                    terms.append(above[p + d - planes])
                                for term in terms:
                                    term = STENCIL[d] * term
                                    value = term if value is None else value + term
                            hs[p, rows, :] = value
            across_y[q].start()

        sum_s.middle()
        halo_part(0)
        sum_s.add()
        sum_c.scatter()
        sum_s.relay()
        sum_c.middle()
        across_z[1].start()
        across_z[2].start()
        across_z[3].start()
        sum_s.finish()
        gather_s.start()
        halo_part(1)
        gather_s.pass_on()
        sum_c.add()
        halo_part(2)
        halo_part(3)
        gather_s.finish()
        for b in range(bands):
            for c in range(bands):
                work[b * w : (b + 1) * w, lanes(c)] = sall[b, c * w : (c + 1) * w, :]

        def exchange_and_send():
            sum_c.relay()
            sum_c.finish()
            coupling = jnp.concatenate(
                [jnp.transpose(csum[c * w : (c + 1) * w, :]) for c in range(bands)], axis=0
            )
            right = split(coupling, 2)
            for copy in across_y:
                copy.wait_recv()

            @pl.loop(0, planes)
            def _(p):
                rows = pl.ds(pl.multiple_of(p * plane, plane), plane)
                exchange = split_dot([xh[rows, :], xm[rows, :]], right, ((1,), (0,)))
                kk[band, p] = kk[band, p] - 0.5 * hr[p] - exchange
            gather_k.start()

        @pl.loop(0, bands)
        def _(k):
            here = pl.ds(pl.multiple_of(k * w, w), w)
            inverse = block_inverse_factor(work[here, here], spread)
            rows = exact_dot(inverse, work[here, :], ((1,), (0,)))
            panel[...] = rows
            work[here, :] = rows
            work[here, here] = inverse

            @pl.loop(k + 1, bands)
            def _(i):
                there = pl.ds(pl.multiple_of(i * w, w), w)
                work[there, here] = jnp.zeros((w, w), F32)
                work[there, :] = work[there, :] - exact_dot(
                    panel[:, there], work[here, :], ((0,), (0,))
                )

            @pl.when(k == 0)
            def _():
                exchange_and_send()

            @pl.when(k == bands - 2)
            def _():
                gather_k.pass_on(0, PIECES // 2)

        gather_k.pass_on(PIECES // 2, PIECES)
        for r in range(bands):
            rows = slice(r * w, (r + 1) * w)
            for target, piece in zip((lh, lm, ll), split(work[rows, :], 3)):
                target[rows, : (r + 1) * w] = piece[:, : (r + 1) * w]
                if (r + 1) * w < total:
                    target[rows, (r + 1) * w :] = jnp.zeros((w, total - (r + 1) * w), BF16)
        gather_k.finish()
        split_blocks(kk, (kh, km))
        for copy in across_z + across_y:
            copy.wait_send()

        @pl.loop(0, planes)
        def _(p):
            rows = pl.ds(pl.multiple_of(p * plane, plane), plane)
            for start in range(0, total, WIDE):
                deep = slice(0, start + WIDE)
                wide = slice(start, start + WIDE)
                right = [lh[wide, deep], lm[wide, deep], ll[wide, deep]]
                v = split_dot([uh[rows, deep], um[rows, deep], ul[rows, deep]], right, ((1,), (1,)))
                t = split_dot([kh[rows, deep], km[rows, deep]], right[:2], ((1,), (1,)))
                for c in range(WIDE // w):
                    u[start // w + c, p] = v[:, lanes(c)]
                    wb[start // w + c, p] = t[:, lanes(c)]

        def column_sum(value):
            return jnp.sum(value, axis=0, keepdims=True)

        def eight(value):
            return jnp.sum(value.reshape(plane // 8, 8, w), axis=0)

        for j in range(bands):
            zero = jnp.zeros((8, w), F32)

            def first(p, carry, j=j):
                v, t = u[j, p], wb[j, p]
                return carry[0] + eight(v * t), carry[1] + eight(v * v)

            vw, vv = lax.fori_loop(0, planes, first, (zero, zero))
            vw, vv = column_sum(vw), column_sum(vv)
            slope = jnp.where(vv > 1e-12, vw / jnp.maximum(vv, 1e-12), 0.0)

            def second(p, carry, j=j, slope=slope):
                r = wb[j, p] - slope * u[j, p]
                return carry + eight(r * r)

            rest = column_sum(lax.fori_loop(0, planes, second, zero))
            stat[j : j + 1, :] = vw
            stat[bands + j : bands + j + 1, :] = vv
            stat[2 * bands + j : 2 * bands + j + 1, :] = rest

        copies = []
        for k, peer in enumerate(peers):
            copy = remote("grid", peer, stat, stats.at[me], stat_s.at[k], stat_r.at[me])
            copy.start()
            copies.append(copy)
        stats[me] = stat[...]
        for k, peer in enumerate(peers):
            remote("grid", peer, stat, stats.at[peer], stat_s.at[k], stat_r.at[peer]).wait_recv()
        for copy in copies:
            copy.wait_send()
        quotient = stats[0, :bands, :]
        for c in range(1, count):
            quotient = quotient + stats[c, :bands, :]
        squared = jnp.zeros((bands, w), F32)
        for c in range(count):
            vw, vv = stats[c, :bands, :], stats[c, bands : 2 * bands, :]
            slope = jnp.where(vv > 1e-12, vw / jnp.maximum(vv, 1e-12), 0.0)
            shift = slope - quotient
            squared = squared + stats[c, 2 * bands : 3 * bands, :]
            squared = squared + shift * (2.0 * (vw - slope * vv) + shift * vv)
        squared = jnp.maximum(squared, 0.0)
        lam[0, :bands, :] = quotient
        lam[1, :bands, :] = jnp.sqrt(squared)
        lam[2, :bands, :] = STEP_LENGTH / jnp.sqrt(squared + NORM_EPS)
        quot_ref[pl.ds(it, 1), :] = lam[0, pl.ds(band, 1), :]
        norm_ref[pl.ds(it, 1), :] = lam[1, pl.ds(band, 1), :]
        for j in range(bands):
            rate, length = lam[0, j : j + 1, :], lam[2, j : j + 1, :]

            @pl.loop(0, planes)
            def _(p, j=j, rate=rate, length=length):
                v = u[j, p]
                u[j, p] = v - (wb[j, p] - rate * v) * length

    @pl.loop(0, ITERS)
    def _(it):
        iteration(it)

    out_ref[...] = u[band]


def local(orbitals, projectors, potential):
    grid_shape = orbitals.shape
    planes, nx, ny, w = grid_shape
    plane = nx * ny
    n = planes * plane
    count = lax.axis_size("grid")
    bands = lax.axis_size("band")
    total = bands * w
    chunk = total // count
    field = (planes, plane, w)
    block = pltpu.VMEM((bands,) + field, F32)
    half = pltpu.VMEM((n, total), BF16)
    square = pltpu.VMEM((total, total), BF16)
    column = pltpu.VMEM((total, w), F32)
    chunks = pltpu.VMEM((count // 2, chunk, w), F32)
    slab = pltpu.VMEM(field, F32)
    dma = pltpu.SemaphoreType.DMA
    spread_potential = jnp.broadcast_to(potential.reshape(planes, plane, 1), field)
    line = jax.ShapeDtypeStruct((ITERS, w), F32)
    updated, quotients, norms = pl.pallas_call(
        functools.partial(iterations_kernel, count, bands, ny),
        out_shape=(jax.ShapeDtypeStruct(field, F32), line, line),
        in_specs=[VMEM] * 3,
        out_specs=(VMEM, VMEM, VMEM),
        scratch_shapes=[block] * 4
        + [half] * 7
        + [square] * 3
        + [
            pltpu.VMEM((total, total), F32),
            pltpu.VMEM((w, total), F32),
            pltpu.VMEM((2, 72, w), F32),
        ]
        + [column, column] + [chunks] * 6 + [column]
        + [pltpu.VMEM((bands, total, w), F32), slab, slab, slab]
        + [
            pltpu.VMEM((16, w), F32),
            pltpu.VMEM((count, 16, w), F32),
            pltpu.VMEM((3, 8, w), F32),
        ]
        + [dma((8, count // 2))] * 2
        + [dma((2, 3, PIECES))] * 4
        + [dma((2, PIECES))] * 2
        + [dma((count,))] * 2,
        compiler_params=pltpu.CompilerParams(
            collective_id=0, has_side_effects=True, vmem_limit_bytes=60 * 2**20
        ),
    )(orbitals.reshape(field), projectors.reshape(field), spread_potential)
    return updated.reshape(grid_shape), quotients, norms


def solution(mesh):
    return jax.shard_map(
        local,
        mesh=mesh,
        in_specs=(
            P("grid", None, None, "band"),
            P("grid", None, None, "band"),
            P("grid", None, None),
        ),
        out_specs=(P("grid", None, None, "band"), P(None, "band"), P(None, "band")),
        check_vma=False,
    )
```

```python
import functools

import jax
import jax.numpy as jnp
from jax import lax
from jax.experimental import pallas as pl
from jax.experimental.pallas import tpu as pltpu
from jax.sharding import PartitionSpec as P

ITERS = 3


STENCIL = (-205.0 / 72.0, 8.0 / 5.0, -1.0 / 5.0, 8.0 / 315.0, -1.0 / 560.0)
STEP_LENGTH = 0.25
NORM_EPS = 1e-06
HIGHEST = lax.Precision.HIGHEST
MESH = pl.DeviceIdType.MESH
VMEM = pl.BlockSpec(memory_space=pltpu.VMEM)
PIECES = 4
WIDE = 256
BF16 = jnp.bfloat16
F32 = jnp.float32


def exact_dot(left, right, contract):
    return lax.dot_general(
        left, right, (contract, ((), ())), precision=HIGHEST, preferred_element_type=F32
    )


def plain_dot(left, right, contract):
    return lax.dot_general(left, right, (contract, ((), ())), preferred_element_type=F32)


def split(value, parts):
    pieces = []
    for _ in range(parts - 1):
        head = value.astype(BF16)
        pieces.append(head)
        value = value - head.astype(F32)
    pieces.append(value.astype(BF16))
    return pieces


def split_dot(left, right, contract):
    total = None
    for order in reversed(range(max(len(left), len(right)))):
        for i in range(order + 1):
            if i < len(left) and order - i < len(right):
                term = plain_dot(left[i], right[order - i], contract)
                total = term if total is None else total + term
    return total


def block_inverse_factor(block, spread):
    size = block.shape[0]
    count = size // 8
    groups = [block[8 * g : 8 * g + 8, :] for g in range(count)]
    lane = lax.broadcasted_iota(jnp.int32, (8, size), 1)
    sublane = lax.broadcasted_iota(jnp.int32, (8, size), 0)

    def spread_column(value, j):
        return jnp.broadcast_to(value[:, j : j + 1], (8, size))

    finished = []
    for g in range(count):
        first = 8 * g
        slot = g % 2
        inside = (lane >= first) & (lane < first + 8)
        for t in range(8):
            spread[slot, 8 * t : 8 * t + 8, :] = spread_column(groups[g], first + t)
        start = jnp.where(inside, jnp.where(lane - first == sublane, 1.0, 0.0), groups[g])
        spread[slot, 64:72, :] = start

        def stored(at):
            return jnp.broadcast_to(spread[slot, at : at + 1, :], (8, size))

        entry = [[stored(8 * t + s) for t in range(s + 1)] for s in range(8)]
        rows = [stored(64 + s) for s in range(8)]
        following = g + 1 < count
        if following:
            ahead = [spread_column(groups[g + 1], first + t) for t in range(8)]
            value = jnp.where(inside, 0.0, groups[g + 1])
        inverse_pivot = []
        factor = [[None] * 8 for _ in range(8)]
        for t in range(8):
            inverse_pivot.append(1.0 / entry[t][t])
            for s in range(t + 1, 8):
                factor[s][t] = entry[s][t] * inverse_pivot[t]
                for u in range(t + 1, s + 1):
                    entry[s][u] = entry[s][u] - factor[s][t] * entry[u][t]
                rows[s] = rows[s] - factor[s][t] * rows[t]
                if following:
                    ahead[s] = ahead[s] - factor[s][t] * ahead[t]
            if following:
                value = value - (ahead[t] * inverse_pivot[t]) * rows[t]
        if following:
            groups[g + 1] = value
        result = jnp.zeros((8, size), F32)
        for s in range(8):
            result = jnp.where(sublane == s, rows[s] * (1.0 / jnp.sqrt(entry[s][s])), result)
        finished.append(jnp.where(lane < first + 8, result, 0.0))
        if g + 2 < count:
            solved = [None] * 8
            for s in reversed(range(8)):
                solved[s] = rows[s] * inverse_pivot[s]
                for t in range(s + 1, 8):
                    solved[s] = solved[s] - factor[t][s] * solved[t]
            for i in range(g + 2, count):
                value = jnp.where(inside, 0.0, groups[i])
                for t in range(8):
                    value = value - spread_column(groups[i], first + t) * solved[t]
                groups[i] = value
    return jnp.concatenate(finished, axis=0)


def remote(axis, peer, source, target, send_sem, recv_sem):
    return pltpu.make_async_remote_copy(
        src_ref=source,
        dst_ref=target,
        send_sem=send_sem,
        recv_sem=recv_sem,
        device_id={axis: peer},
        device_id_type=MESH,
    )


class BandGather:
    def __init__(self, source, target, place, parts, sems):
        send, recv = sems
        me, partner, across = place
        self.copies = []
        for q, part in enumerate(parts):

            def block(owner, part=part):
                return target.at[owner, :, part, :]

            here = source.at[:, part, :]
            far = remote("band", across, here, block(me), send.at[0, q], recv.at[0, q])
            near = remote("band", partner, here, block(me), send.at[1, q], recv.at[1, q])
            relay = remote(
                "band", partner, block(across), block(across), send.at[2, q], recv.at[2, q]
            )
            self.copies.append((far, near, relay))

    def send(self, *which):
        for q in which:
            self.copies[q][0].start()
        for q in which:
            self.copies[q][1].start()

    def pass_on(self, *which):
        for q in which:
            self.copies[q][0].wait_recv()
            self.copies[q][2].start()

    def finish(self):
        for far, near, relay in self.copies:
            near.wait_recv()
            relay.wait_recv()
        for far, near, relay in self.copies:
            far.wait_send()
            near.wait_send()
            relay.wait_send()


def far_first(me, count):
    low = 2 * me < count
    peers = []
    for k in range(count - 1):
        down = count - 1 - k
        down = jnp.where(down > me, down, down - 1)
        up = jnp.where(k < me, k, k + 1)
        peers.append(jnp.where(low, down, up))
    return peers


class GridSum:
    def __init__(self, part, paired, arrived, middle, target, me, count, sems, ready=None):
        pair_s, pair_r, far_s, far_r, back_s, back_r, pass_s, pass_r = sems
        self.part, self.paired, self.arrived, self.held, self.target = (
            part, paired, arrived, middle, target,
        )
        chunk = middle.shape[1]
        half = count // 2
        place, side = lax.div(me, 2), lax.rem(me, 2)
        pair = me + 1 - 2 * side
        self.order = far_first(place, half) + [place]
        self.last = half - 1
        self.ready = ready

        def rows(parity, owner):
            return pl.ds(pl.multiple_of((parity * half + owner) * chunk, chunk), chunk)

        self.mine = [rows(side, owner) for owner in self.order]
        self.parts = self.mine + [rows(1 - side, owner) for owner in self.order]
        self.pairs, self.far, self.far_in, self.back, self.back_in, self.passed = [], [], [], [], [], []
        own = middle.at[self.last]
        for j, owner in enumerate(self.order):
            theirs = part.at[rows(1 - side, owner), :]
            self.pairs.append(
                remote("grid", pair, theirs, paired.at[j], pair_s.at[j], pair_r.at[j])
            )
            done = target.at[self.mine[j], :]
            source = own if j == self.last else done
            self.passed.append(remote("grid", pair, source, done, pass_s.at[j], pass_r.at[j]))
            if j == self.last:
                continue
            peer = 2 * owner + side
            here = middle.at[j]
            self.far.append(
                remote("grid", peer, here, arrived.at[place], far_s.at[j], far_r.at[place])
            )
            self.far_in.append(
                remote("grid", peer, here, arrived.at[owner], far_s.at[j], far_r.at[owner])
            )
            home = target.at[rows(side, place), :]
            self.back.append(remote("grid", peer, own, home, back_s.at[j], back_r.at[place]))
            self.back_in.append(remote("grid", peer, own, done, back_s.at[j], back_r.at[owner]))

    def scatter(self):
        for copy in self.pairs:
            copy.start()

    def middle(self):
        for j, copy in enumerate(self.pairs):
            copy.wait_recv()
            self.held[j] = self.part[self.mine[j], :] + self.paired[j]
            if j < self.last:
                self.far[j].start()

    def add(self):
        total = self.held[self.last]
        for j in reversed(range(self.last)):
            self.far_in[j].wait_recv()
            total = total + self.arrived[self.order[j]]
        self.held[self.last] = total
        for copy in self.back:
            copy.start()
        self.passed[self.last].start()
        self.target[self.mine[self.last], :] = total
        if self.ready:
            self.ready(self.last)

    def relay(self):
        for j in reversed(range(self.last)):
            self.back_in[j].wait_recv()
            self.passed[j].start()
            if self.ready:
                self.ready(j)

    def finish(self):
        for j in reversed(range(self.last + 1)):
            self.passed[j].wait_recv()
            if self.ready:
                self.ready(self.last + 1 + j)
        for copy in self.pairs + self.far + self.back + self.passed:
            copy.wait_send()


def iterations_kernel(count, bands, ny, *refs):
    (u0, x0, pot, out_ref, quot_ref, norm_ref) = refs[:6]
    (
        u, xr, kk, wb, uh, um, ul, xh, xm, kh, km, lh, lm, work, spread,
        spart, cpart, spair, cpair, sin, cin, smid, cmid, csum, sall, hz, hs, hr, stat, stats, lam,
        sums_s, sums_c, gat_u, gat_x, gat_s, gat_k, halo_z, halo_y, stat_s, stat_r,
    ) = refs[6:]
    me = lax.axis_index("grid")
    band = lax.axis_index("band")
    half, side = lax.div(band, 2), lax.rem(band, 2)
    partner = half * 2 + 1 - side
    across = (1 - half) * 2 + side
    place = (band, partner, across)
    planes, plane, w = u0.shape
    n = planes * plane
    total = bands * w
    nx = plane // ny

    barrier = pltpu.get_barrier_semaphore()
    for k in range(1, count):
        pl.semaphore_signal(
            barrier, inc=1, device_id={"grid": lax.rem(me + k, count)}, device_id_type=MESH
        )
    for peer in (partner, across):
        pl.semaphore_signal(barrier, inc=1, device_id={"band": peer}, device_id_type=MESH)
    pl.semaphore_wait(barrier, count + 1)

    stat[...] = jnp.zeros_like(stat)
    part_rows = plane // PIECES
    parts = [pl.ds(q * part_rows, part_rows) for q in range(PIECES)]
    every = range(PIECES)
    gather_u = BandGather(u0, u, place, parts, (gat_u.at[0], gat_u.at[1]))
    gather_x = BandGather(x0, xr, place, parts, (gat_x.at[0], gat_x.at[1]))
    gather_u.send(*every)
    gather_x.send(*every)
    u[band] = u0[...]
    xr[band] = x0[...]
    gather_u.pass_on(*every)
    gather_u.finish()

    peers = far_first(me, count)
    odd = lax.rem(me, 2)
    z_peer = lax.rem(me + count + 4 * odd - 2, count)
    y_peer = me + 1 - 2 * odd

    def lanes(j):
        return slice(j * w, (j + 1) * w)

    def split_blocks(source, targets):
        for j in range(bands):
            @pl.loop(0, planes)
            def _(p):
                rows = pl.ds(pl.multiple_of(p * plane, plane), plane)
                for target, piece in zip(targets, split(source[j, p], len(targets))):
                    target[rows, lanes(j)] = piece

    def iteration(it):
        sum_s = GridSum(spart, spair, sin, smid, sall.at[band], me, count, [sums_s.at[i] for i in range(8)])
        sum_c = GridSum(cpart, cpair, cin, cmid, csum, me, count, [sums_c.at[i] for i in range(8)])
        gather_s = BandGather(
            sall.at[band].reshape(1, total, w), sall.reshape(bands, 1, total, w), place,
            sum_s.parts, (gat_s.at[0], gat_s.at[1]),
        )
        sum_s.ready = gather_s.send
        last = sum_s.last
        first_half = list(reversed(range(last + 1)))
        second_half = [last + 1 + j for j in first_half]
        gather_k = BandGather(kk.at[band], kk, place, parts, (gat_k.at[0], gat_k.at[1]))
        across_z, across_y = [], []
        for q in range(PIECES):
            part = parts[q]
            across_z.append(
                remote("grid", z_peer, u.at[band, :, part, :], hz.at[:, part, :],
                       halo_z.at[0, q], halo_z.at[1, q])
            )
            across_y.append(
                remote("grid", y_peer, hs.at[:, part, :], hr.at[:, part, :],
                       halo_y.at[0, q], halo_y.at[1, q])
            )

        across_z[0].start()
        split_blocks(u, (uh, um, ul))
        turned = split(jnp.transpose(u[band].reshape(n, w)), 3)
        for start in range(0, total, WIDE):
            wide = slice(start, start + WIDE)
            tile = split_dot(turned, [uh[:, wide], um[:, wide], ul[:, wide]], ((1,), (0,)))
            for c in range(WIDE // w):
                at = start + c * w
                spart[at : at + w, :] = tile[:, lanes(c)]
        sum_s.scatter()

        def couple():
            for start in range(0, total, WIDE):
                wide = slice(start, start + WIDE)
                tile = split_dot(turned[:2], [xh[:, wide], xm[:, wide]], ((1,), (0,)))
                for c in range(WIDE // w):
                    at = start + c * w
                    cpart[at : at + w, :] = tile[:, lanes(c)]

        @pl.loop(0, nx)
        def _(x):
            def rows_at(at):
                return pl.ds(pl.multiple_of(lax.rem(at + nx, nx) * ny, ny), ny)

            rows = rows_at(x)
            field = [u[band, p, rows, :] for p in range(planes)]
            for p in range(planes):
                value = 3.0 * STENCIL[0] * field[p]
                for d in range(1, 5):
                    near = u[band, p, rows_at(x + d), :] + u[band, p, rows_at(x - d), :]
                    near = near + pltpu.roll(field[p], d, 0) + pltpu.roll(field[p], ny - d, 0)
                    if p - d >= 0:
                        near = near + field[p - d]
                    if p + d < planes:
                        near = near + field[p + d]
                    value = value + STENCIL[d] * near
                kk[band, p, rows, :] = -0.5 * value + pot[p, rows, :] * field[p]

        def halo_part(q):
            across_z[q].wait_recv()
            for own_above in (0, 1):
                @pl.when(odd == own_above)
                def _():
                    @pl.loop(0, part_rows // 16)
                    def _(r):
                        rows = pl.ds(pl.multiple_of(q * part_rows + r * 16, 16), 16)
                        own = [u[band, j, rows, :] for j in range(planes)]
                        other = [hz[j, rows, :] for j in range(planes)]
                        below, above = (other, own) if own_above else (own, other)
                        for p in range(planes):
                            value = None
                            for d in range(1, 5):
                                terms = []
                                if p - d < 0:
                                    terms.append(below[planes + p - d])
                                if p + d >= planes:
                                    terms.append(above[p + d - planes])
                                for term in terms:
                                    term = STENCIL[d] * term
                                    value = term if value is None else value + term
                            hs[p, rows, :] = value
            across_y[q].start()

        sum_s.middle()

        @pl.when(it > 0)
        def _():
            couple()

        sum_s.add()

        @pl.when(it == 0)
        def _():
            gather_x.pass_on(*every)
            gather_x.finish()
            split_blocks(xr, (xh, xm))
            couple()

        sum_c.scatter()
        halo_part(0)
        sum_s.relay()
        sum_c.middle()
        across_z[1].start()
        sum_s.finish()
        gather_s.pass_on(*first_half)
        gather_s.pass_on(*second_half)
        sum_c.add()
        across_z[2].start()
        across_z[3].start()
        gather_s.finish()
        for b in range(bands):
            for c in range(bands):
                work[b * w : (b + 1) * w, lanes(c)] = sall[b, c * w : (c + 1) * w, :]

        def exchange():
            sum_c.finish()
            coupling = jnp.concatenate(
                [jnp.transpose(csum[c * w : (c + 1) * w, :]) for c in range(bands)], axis=0
            )
            right = split(coupling, 2)

            @pl.loop(0, planes)
            def _(p):
                rows = pl.ds(pl.multiple_of(p * plane, plane), plane)
                change = split_dot([xh[rows, :], xm[rows, :]], right, ((1,), (0,)))
                kk[band, p] = kk[band, p] - change

        def send_k(q):
            across_y[q].wait_recv()
            for p in range(planes):
                kk[band, p, parts[q], :] = kk[band, p, parts[q], :] - 0.5 * hr[p, parts[q], :]
            gather_k.send(q)

        def service(k):
            if k == 0:
                sum_c.relay()
                halo_part(1)
            if k == 1:
                halo_part(2)
                exchange()
                send_k(0)
                send_k(1)
            if k == 2:
                halo_part(3)
                send_k(2)
            if k == 3:
                send_k(3)
                gather_k.pass_on(0, 1)

        def rows_of(k):
            return slice(k * w, (k + 1) * w)

        inverse = block_inverse_factor(work[rows_of(0), rows_of(0)], spread)
        for k in range(bands - 1):
            service(k)
            here, after = rows_of(k), rows_of(k + 1)
            step = exact_dot(inverse, work[here, after], ((1,), (0,)))
            pivot = work[after, after] - exact_dot(step, step, ((0,), (0,)))
            following = block_inverse_factor(pivot, spread)
            rows = exact_dot(inverse, work[here, (k + 1) * w :], ((1,), (0,)))
            left = inverse
            if k:
                left = jnp.concatenate(
                    [exact_dot(inverse, work[here, : k * w], ((1,), (0,))), inverse], axis=1
                )
            work[here, : (k + 1) * w] = left
            for i in range(k + 1, bands):
                turn = rows[:, (i - k - 1) * w : (i - k) * w]
                if i > k + 1:
                    work[rows_of(i), i * w :] = work[rows_of(i), i * w :] - exact_dot(
                        turn, rows[:, (i - k - 1) * w :], ((0,), (0,))
                    )
                if i + 1 < bands and i == k + 1:
                    work[rows_of(i), (i + 1) * w :] = work[rows_of(i), (i + 1) * w :] - exact_dot(
                        turn, rows[:, w:], ((0,), (0,))
                    )
                change = exact_dot(turn, left, ((0,), (0,)))
                if k:
                    work[rows_of(i), : k * w] = work[rows_of(i), : k * w] - change[:, : k * w]
                work[rows_of(i), here] = -change[:, k * w :]
            inverse = following
        service(bands - 1)
        here = rows_of(bands - 1)
        left = exact_dot(inverse, work[here, : (bands - 1) * w], ((1,), (0,)))
        work[here, :] = jnp.concatenate([left, inverse], axis=1)
        for r in range(bands):
            rows = rows_of(r)
            for target, piece in zip((lh, lm), split(work[rows, : (r + 1) * w], 2)):
                target[rows, : (r + 1) * w] = piece
                if (r + 1) * w < total:
                    target[rows, (r + 1) * w :] = jnp.zeros((w, total - (r + 1) * w), BF16)
        gather_k.pass_on(2, 3)
        gather_k.finish()
        split_blocks(kk, (kh, km))
        for copy in across_z + across_y:
            copy.wait_send()

        def column_sum(value):
            return jnp.sum(value, axis=0, keepdims=True)

        def eight(value):
            return jnp.sum(value.reshape(plane // 8, 8, w), axis=0)

        def apply(p, sums, which, places, deep):
            rows = pl.ds(pl.multiple_of(p * plane, plane), plane)
            right = [lh[which, deep], lm[which, deep]]
            v = split_dot([uh[rows, deep], um[rows, deep]], right, ((1,), (1,)))
            t = split_dot([kh[rows, deep], km[rows, deep]], right, ((1,), (1,)))
            out = []
            for c, (j, (vw, vv)) in enumerate(zip(places, sums)):
                vj, tj = v[:, lanes(c)], t[:, lanes(c)]
                u[j, p] = vj
                wb[j, p] = tj
                out.append((vw + eight(vj * tj), vv + eight(vj * vj)))
            return out

        def record(j, vw, vv):
            vw, vv = column_sum(vw), column_sum(vv)
            slope = jnp.where(vv > 1e-12, vw / jnp.maximum(vv, 1e-12), 0.0)

            def second(p, carry):
                r = wb[j, p] - slope * u[j, p]
                return carry + eight(r * r)

            rest = column_sum(lax.fori_loop(0, planes, second, zero))
            stat[pl.ds(j, 1), :] = vw
            stat[pl.ds(bands + j, 1), :] = vv
            stat[pl.ds(2 * bands + j, 1), :] = rest

        zero = jnp.zeros((8, w), F32)

        @pl.when(it < ITERS - 1)
        def _():
            def body(p, sums):
                out = []
                for start in range(0, total, WIDE):
                    places = range(start // w, (start + WIDE) // w)
                    out += apply(
                        p, [sums[j] for j in places], slice(start, start + WIDE), places,
                        slice(0, start + WIDE),
                    )
                return tuple(out)

            sums = lax.fori_loop(0, planes, body, ((zero, zero),) * bands)
            for j in range(bands):
                record(j, *sums[j])

        @pl.when(it == ITERS - 1)
        def _():
            which = pl.ds(pl.multiple_of(band * w, w), w)

            def body(p, sums):
                return apply(p, [sums], which, [band], slice(0, total))[0]

            vw, vv = lax.fori_loop(0, planes, body, (zero, zero))
            record(band, vw, vv)

        copies = []
        for k, peer in enumerate(peers):
            copy = remote("grid", peer, stat, stats.at[me], stat_s.at[k], stat_r.at[me])
            copy.start()
            copies.append(copy)
        stats[me] = stat[...]
        for k, peer in enumerate(peers):
            remote("grid", peer, stat, stats.at[peer], stat_s.at[k], stat_r.at[peer]).wait_recv()
        for copy in copies:
            copy.wait_send()
        quotient = stats[0, :bands, :]
        for c in range(1, count):
            quotient = quotient + stats[c, :bands, :]
        squared = jnp.zeros((bands, w), F32)
        for c in range(count):
            vw, vv = stats[c, :bands, :], stats[c, bands : 2 * bands, :]
            slope = jnp.where(vv > 1e-12, vw / jnp.maximum(vv, 1e-12), 0.0)
            shift = slope - quotient
            squared = squared + stats[c, 2 * bands : 3 * bands, :]
            squared = squared + shift * (2.0 * (vw - slope * vv) + shift * vv)
        squared = jnp.maximum(squared, 0.0)
        lam[0, :bands, :] = quotient
        lam[1, :bands, :] = jnp.sqrt(squared)
        lam[2, :bands, :] = STEP_LENGTH / jnp.sqrt(squared + NORM_EPS)
        quot_ref[pl.ds(it, 1), :] = lam[0, pl.ds(band, 1), :]
        norm_ref[pl.ds(it, 1), :] = lam[1, pl.ds(band, 1), :]
        def renew(j):
            rate, length = lam[0, pl.ds(j, 1), :], lam[2, pl.ds(j, 1), :]

            @pl.loop(0, planes)
            def _(p):
                v = u[j, p]
                u[j, p] = v - (wb[j, p] - rate * v) * length

        @pl.when(it < ITERS - 1)
        def _():
            for j in range(bands):
                renew(j)

        @pl.when(it == ITERS - 1)
        def _():
            renew(band)

    @pl.loop(0, ITERS)
    def _(it):
        iteration(it)

    out_ref[...] = u[band]


def local(orbitals, projectors, potential):
    grid_shape = orbitals.shape
    planes, nx, ny, w = grid_shape
    plane = nx * ny
    n = planes * plane
    count = lax.axis_size("grid")
    bands = lax.axis_size("band")
    total = bands * w
    chunk = total // count
    field = (planes, plane, w)
    block = pltpu.VMEM((bands,) + field, F32)
    half = pltpu.VMEM((n, total), BF16)
    square = pltpu.VMEM((total, total), BF16)
    column = pltpu.VMEM((total, w), F32)
    chunks = pltpu.VMEM((count // 2, chunk, w), F32)
    slab = pltpu.VMEM(field, F32)
    dma = pltpu.SemaphoreType.DMA
    spread_potential = jnp.broadcast_to(potential.reshape(planes, plane, 1), field)
    line = jax.ShapeDtypeStruct((ITERS, w), F32)
    updated, quotients, norms = pl.pallas_call(
        functools.partial(iterations_kernel, count, bands, ny),
        out_shape=(jax.ShapeDtypeStruct(field, F32), line, line),
        in_specs=[VMEM] * 3,
        out_specs=(VMEM, VMEM, VMEM),
        scratch_shapes=[block] * 4
        + [half] * 7
        + [square] * 2
        + [
            pltpu.VMEM((total, total), F32),
            pltpu.VMEM((2, 72, w), F32),
        ]
        + [column, column] + [chunks] * 6 + [column]
        + [pltpu.VMEM((bands, total, w), F32), slab, slab, slab]
        + [
            pltpu.VMEM((16, w), F32),
            pltpu.VMEM((count, 16, w), F32),
            pltpu.VMEM((3, 8, w), F32),
        ]
        + [dma((8, count // 2))] * 2
        + [dma((2, 3, PIECES))] * 2
        + [dma((2, 3, count)), dma((2, 3, PIECES))]
        + [dma((2, PIECES))] * 2
        + [dma((count,))] * 2,
        compiler_params=pltpu.CompilerParams(
            collective_id=0, has_side_effects=True, vmem_limit_bytes=60 * 2**20
        ),
    )(orbitals.reshape(field), projectors.reshape(field), spread_potential)
    return updated.reshape(grid_shape), quotients, norms


def solution(mesh):
    return jax.shard_map(
        local,
        mesh=mesh,
        in_specs=(
            P("grid", None, None, "band"),
            P("grid", None, None, "band"),
            P("grid", None, None),
        ),
        out_specs=(P("grid", None, None, "band"), P(None, "band"), P(None, "band")),
        check_vma=False,
    )
```

```python
import functools

import jax
import jax.numpy as jnp
from jax import lax
from jax.experimental import pallas as pl
from jax.experimental.pallas import tpu as pltpu
from jax.sharding import PartitionSpec as P

ITERS = 3


STENCIL = (-205.0 / 72.0, 8.0 / 5.0, -1.0 / 5.0, 8.0 / 315.0, -1.0 / 560.0)
STEP_LENGTH = 0.25
NORM_EPS = 1e-06
HIGHEST = lax.Precision.HIGHEST
MESH = pl.DeviceIdType.MESH
VMEM = pl.BlockSpec(memory_space=pltpu.VMEM)
PIECES = 4
WIDE = 256
BF16 = jnp.bfloat16
F32 = jnp.float32


def exact_dot(left, right, contract):
    return lax.dot_general(
        left, right, (contract, ((), ())), precision=HIGHEST, preferred_element_type=F32
    )


def plain_dot(left, right, contract):
    return lax.dot_general(left, right, (contract, ((), ())), preferred_element_type=F32)


def split(value, parts):
    pieces = []
    for _ in range(parts - 1):
        head = value.astype(BF16)
        pieces.append(head)
        value = value - head.astype(F32)
    pieces.append(value.astype(BF16))
    return pieces


def split_dot(left, right, contract):
    total = None
    for order in reversed(range(max(len(left), len(right)))):
        for i in range(order + 1):
            if i < len(left) and order - i < len(right):
                term = plain_dot(left[i], right[order - i], contract)
                total = term if total is None else total + term
    return total


def block_inverse_factor(block, spread, pause):
    size = block.shape[0]
    count = size // 8
    groups = [block[8 * g : 8 * g + 8, :] for g in range(count)]
    lane = lax.broadcasted_iota(jnp.int32, (8, size), 1)
    sublane = lax.broadcasted_iota(jnp.int32, (8, size), 0)

    def spread_column(value, j):
        return jnp.broadcast_to(value[:, j : j + 1], (8, size))

    finished = []
    for g in range(count):
        if g == count // 2:
            pause()
        first = 8 * g
        slot = g % 2
        inside = (lane >= first) & (lane < first + 8)
        for t in range(8):
            spread[slot, 8 * t : 8 * t + 8, :] = spread_column(groups[g], first + t)
        start = jnp.where(inside, jnp.where(lane - first == sublane, 1.0, 0.0), groups[g])
        spread[slot, 64:72, :] = start

        def stored(at):
            return jnp.broadcast_to(spread[slot, at : at + 1, :], (8, size))

        entry = [[stored(8 * t + s) for t in range(s + 1)] for s in range(8)]
        rows = [stored(64 + s) for s in range(8)]
        following = g + 1 < count
        if following:
            ahead = [spread_column(groups[g + 1], first + t) for t in range(8)]
            value = jnp.where(inside, 0.0, groups[g + 1])
        inverse_pivot = []
        factor = [[None] * 8 for _ in range(8)]
        for t in range(8):
            inverse_pivot.append(1.0 / entry[t][t])
            for s in range(t + 1, 8):
                factor[s][t] = entry[s][t] * inverse_pivot[t]
                for u in range(t + 1, s + 1):
                    entry[s][u] = entry[s][u] - factor[s][t] * entry[u][t]
                rows[s] = rows[s] - factor[s][t] * rows[t]
                if following:
                    ahead[s] = ahead[s] - factor[s][t] * ahead[t]
            if following:
                value = value - (ahead[t] * inverse_pivot[t]) * rows[t]
        if following:
            groups[g + 1] = value
        result = jnp.zeros((8, size), F32)
        for s in range(8):
            result = jnp.where(sublane == s, rows[s] * (1.0 / jnp.sqrt(entry[s][s])), result)
        finished.append(jnp.where(lane < first + 8, result, 0.0))
        if g + 2 < count:
            solved = [None] * 8
            for s in reversed(range(8)):
                solved[s] = rows[s] * inverse_pivot[s]
                for t in range(s + 1, 8):
                    solved[s] = solved[s] - factor[t][s] * solved[t]
            for i in range(g + 2, count):
                value = jnp.where(inside, 0.0, groups[i])
                for t in range(8):
                    value = value - spread_column(groups[i], first + t) * solved[t]
                groups[i] = value
    return jnp.concatenate(finished, axis=0)


def remote(axis, peer, source, target, send_sem, recv_sem):
    return pltpu.make_async_remote_copy(
        src_ref=source,
        dst_ref=target,
        send_sem=send_sem,
        recv_sem=recv_sem,
        device_id={axis: peer},
        device_id_type=MESH,
    )


class BandGather:
    def __init__(self, source, target, place, parts, sems):
        send, recv = sems
        me, partner, across = place
        self.copies = []
        for q, part in enumerate(parts):

            def block(owner, part=part):
                return target.at[owner, :, part, :]

            here = source.at[:, part, :]
            far = remote("band", across, here, block(me), send.at[0, q], recv.at[0, q])
            near = remote("band", partner, here, block(me), send.at[1, q], recv.at[1, q])
            relay = remote(
                "band", partner, block(across), block(across), send.at[2, q], recv.at[2, q]
            )
            self.copies.append((far, near, relay))

    def send(self, *which):
        for q in which:
            self.copies[q][0].start()
        for q in which:
            self.copies[q][1].start()

    def pass_on(self, *which):
        for q in which:
            self.copies[q][0].wait_recv()
            self.copies[q][2].start()

    def finish(self):
        for far, near, relay in self.copies:
            near.wait_recv()
            relay.wait_recv()
        for far, near, relay in self.copies:
            far.wait_send()
            near.wait_send()
            relay.wait_send()


def far_first(me, count):
    low = 2 * me < count
    peers = []
    for k in range(count - 1):
        down = count - 1 - k
        down = jnp.where(down > me, down, down - 1)
        up = jnp.where(k < me, k, k + 1)
        peers.append(jnp.where(low, down, up))
    return peers


class GridSum:
    def __init__(self, part, paired, arrived, middle, target, me, count, sems, ready=None):
        pair_s, pair_r, far_s, far_r, back_s, back_r, pass_s, pass_r = sems
        self.part, self.paired, self.arrived, self.held, self.target = (
            part, paired, arrived, middle, target,
        )
        chunk = middle.shape[1]
        half = count // 2
        place, side = lax.div(me, 2), lax.rem(me, 2)
        pair = me + 1 - 2 * side
        self.order = far_first(place, half) + [place]
        self.last = half - 1
        self.ready = ready

        def rows(parity, owner):
            return pl.ds(pl.multiple_of((parity * half + owner) * chunk, chunk), chunk)

        self.mine = [rows(side, owner) for owner in self.order]
        self.parts = self.mine + [rows(1 - side, owner) for owner in self.order]
        self.pairs, self.far, self.far_in, self.back, self.back_in, self.passed = [], [], [], [], [], []
        own = middle.at[self.last]
        for j, owner in enumerate(self.order):
            theirs = part.at[rows(1 - side, owner), :]
            self.pairs.append(
                remote("grid", pair, theirs, paired.at[j], pair_s.at[j], pair_r.at[j])
            )
            done = target.at[self.mine[j], :]
            source = own if j == self.last else done
            self.passed.append(remote("grid", pair, source, done, pass_s.at[j], pass_r.at[j]))
            if j == self.last:
                continue
            peer = 2 * owner + side
            here = middle.at[j]
            self.far.append(
                remote("grid", peer, here, arrived.at[place], far_s.at[j], far_r.at[place])
            )
            self.far_in.append(
                remote("grid", peer, here, arrived.at[owner], far_s.at[j], far_r.at[owner])
            )
            home = target.at[rows(side, place), :]
            self.back.append(remote("grid", peer, own, home, back_s.at[j], back_r.at[place]))
            self.back_in.append(remote("grid", peer, own, done, back_s.at[j], back_r.at[owner]))

    def scatter(self):
        for copy in self.pairs:
            copy.start()

    def middle(self):
        for j, copy in enumerate(self.pairs):
            copy.wait_recv()
            self.held[j] = self.part[self.mine[j], :] + self.paired[j]
            if j < self.last:
                self.far[j].start()

    def add(self):
        total = self.held[self.last]
        for j in reversed(range(self.last)):
            self.far_in[j].wait_recv()
            total = total + self.arrived[self.order[j]]
        self.held[self.last] = total
        for copy in self.back:
            copy.start()
        self.passed[self.last].start()
        self.target[self.mine[self.last], :] = total
        if self.ready:
            self.ready(self.last)

    def relay(self):
        for j in reversed(range(self.last)):
            self.back_in[j].wait_recv()
            self.passed[j].start()
            if self.ready:
                self.ready(j)

    def finish(self):
        for j in reversed(range(self.last + 1)):
            self.passed[j].wait_recv()
            if self.ready:
                self.ready(self.last + 1 + j)
        for copy in self.pairs + self.far + self.back + self.passed:
            copy.wait_send()


def iterations_kernel(count, bands, ny, *refs):
    (u0, x0, pot, out_ref, quot_ref, norm_ref) = refs[:6]
    (
        u, xr, kk, wb, uh, um, ul, xh, xm, kh, km, lh, lm, mh, mm, gh, gm, work, spread,
        spart, cpart, spair, cpair, sin, cin, smid, cmid, call, sall, hz, hs, hr, stat, stats, lam,
        sums_s, sums_c, gat_u, gat_x, gat_s, gat_c, gat_k, halo_z, halo_y, stat_s, stat_r,
    ) = refs[6:]
    me = lax.axis_index("grid")
    band = lax.axis_index("band")
    half, side = lax.div(band, 2), lax.rem(band, 2)
    partner = half * 2 + 1 - side
    across = (1 - half) * 2 + side
    place = (band, partner, across)
    planes, plane, w = u0.shape
    n = planes * plane
    total = bands * w
    nx = plane // ny

    barrier = pltpu.get_barrier_semaphore()
    for k in range(1, count):
        pl.semaphore_signal(
            barrier, inc=1, device_id={"grid": lax.rem(me + k, count)}, device_id_type=MESH
        )
    for peer in (partner, across):
        pl.semaphore_signal(barrier, inc=1, device_id={"band": peer}, device_id_type=MESH)
    pl.semaphore_wait(barrier, count + 1)

    stat[...] = jnp.zeros_like(stat)
    part_rows = plane // PIECES
    parts = [pl.ds(q * part_rows, part_rows) for q in range(PIECES)]
    every = range(PIECES)
    gather_u = BandGather(u0, u, place, parts, (gat_u.at[0], gat_u.at[1]))
    gather_x = BandGather(x0, xr, place, parts, (gat_x.at[0], gat_x.at[1]))
    gather_u.send(*every)
    gather_x.send(*every)
    u[band] = u0[...]
    xr[band] = x0[...]
    gather_u.pass_on(*every)
    gather_u.finish()

    peers = far_first(me, count)
    odd = lax.rem(me, 2)
    z_peer = lax.rem(me + count + 4 * odd - 2, count)
    y_peer = me + 1 - 2 * odd

    def lanes(j):
        return slice(j * w, (j + 1) * w)

    def split_blocks(source, targets):
        for j in range(bands):
            @pl.loop(0, planes)
            def _(p):
                rows = pl.ds(pl.multiple_of(p * plane, plane), plane)
                for target, piece in zip(targets, split(source[j, p], len(targets))):
                    target[rows, lanes(j)] = piece

    def iteration(it):
        sum_s = GridSum(spart, spair, sin, smid, sall.at[band], me, count, [sums_s.at[i] for i in range(8)])
        sum_c = GridSum(cpart, cpair, cin, cmid, call.at[band], me, count, [sums_c.at[i] for i in range(8)])
        gather_s = BandGather(
            sall.at[band].reshape(1, total, w), sall.reshape(bands, 1, total, w), place,
            sum_s.parts, (gat_s.at[0], gat_s.at[1]),
        )
        sum_s.ready = gather_s.send
        last = sum_s.last
        first_half = list(reversed(range(last + 1)))
        second_half = [last + 1 + j for j in first_half]
        gather_c = BandGather(
            call.at[band].reshape(1, total, w), call.reshape(bands, 1, total, w), place,
            sum_c.parts, (gat_c.at[0], gat_c.at[1]),
        )
        gather_k = BandGather(kk.at[band], kk, place, parts, (gat_k.at[0], gat_k.at[1]))
        across_z, across_y = [], []
        for q in range(PIECES):
            part = parts[q]
            across_z.append(
                remote("grid", z_peer, u.at[band, :, part, :], hz.at[:, part, :],
                       halo_z.at[0, q], halo_z.at[1, q])
            )
            across_y.append(
                remote("grid", y_peer, hs.at[:, part, :], hr.at[:, part, :],
                       halo_y.at[0, q], halo_y.at[1, q])
            )

        across_z[0].start()
        split_blocks(u, (uh, um, ul))
        turned = split(jnp.transpose(u[band].reshape(n, w)), 3)
        for start in range(0, total, WIDE):
            wide = slice(start, start + WIDE)
            tile = split_dot(turned, [uh[:, wide], um[:, wide], ul[:, wide]], ((1,), (0,)))
            for c in range(WIDE // w):
                at = start + c * w
                spart[at : at + w, :] = tile[:, lanes(c)]
        sum_s.scatter()

        def couple():
            for start in range(0, total, WIDE):
                wide = slice(start, start + WIDE)
                tile = split_dot(turned[:2], [xh[:, wide], xm[:, wide]], ((1,), (0,)))
                for c in range(WIDE // w):
                    at = start + c * w
                    cpart[at : at + w, :] = tile[:, lanes(c)]

        @pl.loop(0, nx)
        def _(x):
            def rows_at(at):
                return pl.ds(pl.multiple_of(lax.rem(at + nx, nx) * ny, ny), ny)

            rows = rows_at(x)
            field = [u[band, p, rows, :] for p in range(planes)]
            for p in range(planes):
                value = 3.0 * STENCIL[0] * field[p]
                for d in range(1, 5):
                    near = u[band, p, rows_at(x + d), :] + u[band, p, rows_at(x - d), :]
                    near = near + pltpu.roll(field[p], d, 0) + pltpu.roll(field[p], ny - d, 0)
                    if p - d >= 0:
                        near = near + field[p - d]
                    if p + d < planes:
                        near = near + field[p + d]
                    value = value + STENCIL[d] * near
                kk[band, p, rows, :] = -0.5 * value + pot[p, rows, :] * field[p]

        def halo_part(q):
            across_z[q].wait_recv()
            for own_above in (0, 1):
                @pl.when(odd == own_above)
                def _():
                    @pl.loop(0, part_rows // 16)
                    def _(r):
                        rows = pl.ds(pl.multiple_of(q * part_rows + r * 16, 16), 16)
                        own = [u[band, j, rows, :] for j in range(planes)]
                        other = [hz[j, rows, :] for j in range(planes)]
                        below, above = (other, own) if own_above else (own, other)
                        for p in range(planes):
                            value = None
                            for d in range(1, 5):
                                terms = []
                                if p - d < 0:
                                    terms.append(below[planes + p - d])
                                if p + d >= planes:
                                    terms.append(above[p + d - planes])
                                for term in terms:
                                    term = STENCIL[d] * term
                                    value = term if value is None else value + term
                            hs[p, rows, :] = value
            across_y[q].start()

        sum_s.middle()

        @pl.when(it > 0)
        def _():
            couple()

        sum_s.add()

        @pl.when(it == 0)
        def _():
            gather_x.pass_on(*every)
            gather_x.finish()
            split_blocks(xr, (xh, xm))
            couple()

        sum_c.scatter()
        halo_part(0)
        sum_s.relay()
        sum_c.middle()
        across_z[1].start()
        across_z[2].start()
        sum_s.finish()
        gather_s.pass_on(*first_half)
        gather_s.pass_on(*second_half)
        sum_c.add()
        across_z[3].start()
        gather_s.finish()
        for b in range(bands):
            for c in range(bands):
                work[b * w : (b + 1) * w, lanes(c)] = sall[b, c * w : (c + 1) * w, :]

        def send_k(q):
            across_y[q].wait_recv()
            for p in range(planes):
                kk[band, p, parts[q], :] = kk[band, p, parts[q], :] - 0.5 * hr[p, parts[q], :]
            gather_k.send(q)

        def service(k):
            if k == 0:
                halo_part(1)
            if k == 1:
                sum_c.ready = gather_c.send
                gather_c.send(last)
                sum_c.relay()
                send_k(0)
                halo_part(2)
            if k == 2:
                halo_part(3)
            if k == 3:
                sum_c.finish()
                send_k(1)
            if k == 4:
                send_k(2)
                gather_c.pass_on(*first_half)
            if k == 5:
                gather_c.pass_on(*second_half)
                send_k(3)
            if k == 6:
                gather_k.pass_on(0, 1)
            if k == 7:
                gather_k.pass_on(2)
                gather_c.finish()

        def rows_of(k):
            return slice(k * w, (k + 1) * w)

        inverse = block_inverse_factor(
            work[rows_of(0), rows_of(0)], spread, functools.partial(service, 0)
        )
        for k in range(bands - 1):
            service(2 * k + 1)
            here, after = rows_of(k), rows_of(k + 1)
            step = exact_dot(inverse, work[here, after], ((1,), (0,)))
            pivot = work[after, after] - exact_dot(step, step, ((0,), (0,)))
            rows = exact_dot(inverse, work[here, (k + 1) * w :], ((1,), (0,)))
            left = inverse
            if k:
                left = jnp.concatenate(
                    [exact_dot(inverse, work[here, : k * w], ((1,), (0,))), inverse], axis=1
                )
            work[here, : (k + 1) * w] = left
            for i in range(k + 1, bands):
                turn = rows[:, (i - k - 1) * w : (i - k) * w]
                begin = max(i, k + 2)
                if begin < bands:
                    work[rows_of(i), begin * w :] = work[rows_of(i), begin * w :] - exact_dot(
                        turn, rows[:, (begin - k - 1) * w :], ((0,), (0,))
                    )
                change = exact_dot(turn, left, ((0,), (0,)))
                if k:
                    work[rows_of(i), : k * w] = work[rows_of(i), : k * w] - change[:, : k * w]
                work[rows_of(i), here] = -change[:, k * w :]
            inverse = block_inverse_factor(pivot, spread, functools.partial(service, 2 * k + 2))
        service(2 * bands - 1)
        here = rows_of(bands - 1)
        left = exact_dot(inverse, work[here, : (bands - 1) * w], ((1,), (0,)))
        work[here, :] = jnp.concatenate([left, inverse], axis=1)
        for r in range(bands):
            rows = rows_of(r)
            for target, piece in zip((lh, lm), split(work[rows, : (r + 1) * w], 2)):
                target[rows, : (r + 1) * w] = piece
                if (r + 1) * w < total:
                    target[rows, (r + 1) * w :] = jnp.zeros((w, total - (r + 1) * w), BF16)
            for c in range(bands):
                for target, piece in zip((mh, mm), split(call[r, c * w : (c + 1) * w, :], 2)):
                    target[rows, lanes(c)] = piece
        for start in range(0, total, WIDE):
            wide, deep = slice(start, start + WIDE), slice(0, start + WIDE)
            tile = split_dot(
                [lh[wide, deep], lm[wide, deep]], [mh[deep, :], mm[deep, :]], ((1,), (0,))
            )
            gh[wide, :], gm[wide, :] = split(tile, 2)
        gather_k.pass_on(3)
        gather_k.finish()
        split_blocks(kk, (kh, km))
        for copy in across_z + across_y:
            copy.wait_send()

        def column_sum(value):
            return jnp.sum(value, axis=0, keepdims=True)

        def eight(value):
            return jnp.sum(value.reshape(plane // 8, 8, w), axis=0)

        def apply(p, sums, which, places, deep):
            rows = pl.ds(pl.multiple_of(p * plane, plane), plane)
            right = [lh[which, deep], lm[which, deep]]
            v = split_dot([uh[rows, deep], um[rows, deep]], right, ((1,), (1,)))
            t = split_dot([kh[rows, deep], km[rows, deep]], right, ((1,), (1,)))
            coupled = [gh[which, :], gm[which, :]]
            t = t - split_dot([xh[rows, :], xm[rows, :]], coupled, ((1,), (1,)))
            out = []
            for c, (j, (vw, vv)) in enumerate(zip(places, sums)):
                vj, tj = v[:, lanes(c)], t[:, lanes(c)]
                u[j, p] = vj
                wb[j, p] = tj
                out.append((vw + eight(vj * tj), vv + eight(vj * vj)))
            return out

        def record(j, vw, vv):
            vw, vv = column_sum(vw), column_sum(vv)
            slope = jnp.where(vv > 1e-12, vw / jnp.maximum(vv, 1e-12), 0.0)

            def second(p, carry):
                r = wb[j, p] - slope * u[j, p]
                return carry + eight(r * r)

            rest = column_sum(lax.fori_loop(0, planes, second, zero))
            stat[pl.ds(j, 1), :] = vw
            stat[pl.ds(bands + j, 1), :] = vv
            stat[pl.ds(2 * bands + j, 1), :] = rest

        zero = jnp.zeros((8, w), F32)

        @pl.when(it < ITERS - 1)
        def _():
            def body(p, sums):
                out = []
                for start in range(0, total, WIDE):
                    places = range(start // w, (start + WIDE) // w)
                    out += apply(
                        p, [sums[j] for j in places], slice(start, start + WIDE), places,
                        slice(0, start + WIDE),
                    )
                return tuple(out)

            sums = lax.fori_loop(0, planes, body, ((zero, zero),) * bands)
            for j in range(bands):
                record(j, *sums[j])

        @pl.when(it == ITERS - 1)
        def _():
            which = pl.ds(pl.multiple_of(band * w, w), w)

            def body(p, sums):
                return apply(p, [sums], which, [band], slice(0, total))[0]

            vw, vv = lax.fori_loop(0, planes, body, (zero, zero))
            record(band, vw, vv)

        copies = []
        for k, peer in enumerate(peers):
            copy = remote("grid", peer, stat, stats.at[me], stat_s.at[k], stat_r.at[me])
            copy.start()
            copies.append(copy)
        stats[me] = stat[...]
        for k, peer in enumerate(peers):
            remote("grid", peer, stat, stats.at[peer], stat_s.at[k], stat_r.at[peer]).wait_recv()
        for copy in copies:
            copy.wait_send()
        quotient = stats[0, :bands, :]
        for c in range(1, count):
            quotient = quotient + stats[c, :bands, :]
        squared = jnp.zeros((bands, w), F32)
        for c in range(count):
            vw, vv = stats[c, :bands, :], stats[c, bands : 2 * bands, :]
            slope = jnp.where(vv > 1e-12, vw / jnp.maximum(vv, 1e-12), 0.0)
            shift = slope - quotient
            squared = squared + stats[c, 2 * bands : 3 * bands, :]
            squared = squared + shift * (2.0 * (vw - slope * vv) + shift * vv)
        squared = jnp.maximum(squared, 0.0)
        lam[0, :bands, :] = quotient
        lam[1, :bands, :] = jnp.sqrt(squared)
        lam[2, :bands, :] = STEP_LENGTH / jnp.sqrt(squared + NORM_EPS)
        quot_ref[pl.ds(it, 1), :] = lam[0, pl.ds(band, 1), :]
        norm_ref[pl.ds(it, 1), :] = lam[1, pl.ds(band, 1), :]
        def renew(j):
            rate, length = lam[0, pl.ds(j, 1), :], lam[2, pl.ds(j, 1), :]

            @pl.loop(0, planes)
            def _(p):
                v = u[j, p]
                u[j, p] = v - (wb[j, p] - rate * v) * length

        @pl.when(it < ITERS - 1)
        def _():
            for j in range(bands):
                renew(j)

        @pl.when(it == ITERS - 1)
        def _():
            renew(band)

    @pl.loop(0, ITERS)
    def _(it):
        iteration(it)

    out_ref[...] = u[band]


def local(orbitals, projectors, potential):
    grid_shape = orbitals.shape
    planes, nx, ny, w = grid_shape
    plane = nx * ny
    n = planes * plane
    count = lax.axis_size("grid")
    bands = lax.axis_size("band")
    total = bands * w
    chunk = total // count
    field = (planes, plane, w)
    block = pltpu.VMEM((bands,) + field, F32)
    half = pltpu.VMEM((n, total), BF16)
    square = pltpu.VMEM((total, total), BF16)
    column = pltpu.VMEM((total, w), F32)
    chunks = pltpu.VMEM((count // 2, chunk, w), F32)
    slab = pltpu.VMEM(field, F32)
    dma = pltpu.SemaphoreType.DMA
    spread_potential = jnp.broadcast_to(potential.reshape(planes, plane, 1), field)
    line = jax.ShapeDtypeStruct((ITERS, w), F32)
    updated, quotients, norms = pl.pallas_call(
        functools.partial(iterations_kernel, count, bands, ny),
        out_shape=(jax.ShapeDtypeStruct(field, F32), line, line),
        in_specs=[VMEM] * 3,
        out_specs=(VMEM, VMEM, VMEM),
        scratch_shapes=[block] * 4
        + [half] * 7
        + [square] * 6
        + [
            pltpu.VMEM((total, total), F32),
            pltpu.VMEM((2, 72, w), F32),
        ]
        + [column, column] + [chunks] * 6
        + [pltpu.VMEM((bands, total, w), F32)] * 2
        + [slab, slab, slab]
        + [
            pltpu.VMEM((16, w), F32),
            pltpu.VMEM((count, 16, w), F32),
            pltpu.VMEM((3, 8, w), F32),
        ]
        + [dma((8, count // 2))] * 2
        + [dma((2, 3, PIECES))] * 2
        + [dma((2, 3, count))] * 2
        + [dma((2, 3, PIECES))]
        + [dma((2, PIECES))] * 2
        + [dma((count,))] * 2,
        compiler_params=pltpu.CompilerParams(
            collective_id=0, has_side_effects=True, vmem_limit_bytes=60 * 2**20
        ),
    )(orbitals.reshape(field), projectors.reshape(field), spread_potential)
    return updated.reshape(grid_shape), quotients, norms


def solution(mesh):
    return jax.shard_map(
        local,
        mesh=mesh,
        in_specs=(
            P("grid", None, None, "band"),
            P("grid", None, None, "band"),
            P("grid", None, None),
        ),
        out_specs=(P("grid", None, None, "band"), P(None, "band"), P(None, "band")),
        check_vma=False,
    )
```
